256 devices in a mesh: gy: 16 (over y, x_hi, core), gx: 16 (over z, x_lo).
Axes of the slice: x: 4 (x_hi: 2, x_lo: 2; x = x_hi * 2 + x_lo), y: 4, z: 8, core: 2. Of those that a mesh axis runs over, the one named last changes fastest.
Arguments:
- ice_velocity: float32 [2, 3584, 2048], P(None, 'gy', 'gx'), may hold values from -6 to 6
- ice_stress: float32 [3, 3584, 2048], P(None, 'gy', 'gx'), may hold values from -3 to 3
- ice_mass: float32 [3584, 2048], P('gy', 'gx'), may hold values from 0.5 to 4
- ice_strength: float32 [3584, 2048], P('gy', 'gx'), may hold values from 0.5 to 4
- wind_stress: float32 [2, 3584, 2048], P(None, 'gy', 'gx'), may hold values from -3 to 3
- sea_level: float32 [3584, 2048], P('gy', 'gx'), may hold values from -3 to 3
- transport: float32 [2, 3584, 2048], P(None, 'gy', 'gx'), may hold values from -6 to 6
- depth: float32 [3584, 2048], P('gy', 'gx'), may hold values from 0.5 to 2
- land_mask: int32 [3584, 2048], P('gy', 'gx'), may hold values 0 or 1
- ice_mask: int32 [3584, 2048], P('gy', 'gx'), may hold values 0 or 1
- fold_partner: int32 [2048], P('gx'), may hold values from 0 to 2047, as said below
Outputs:
- ice_velocity_out: float32 [2, 3584, 2048], P(None, 'gy', 'gx')
- ice_stress_out: float32 [3, 3584, 2048], P(None, 'gy', 'gx')
- sea_level_out: float32 [3584, 2048], P('gy', 'gx')
- transport_out: float32 [2, 3584, 2048], P(None, 'gy', 'gx')
The draws below stay inside these ranges and needn't reach their ends.
Inputs may be any that keep to these rules, and one draw needn't show every extreme that they name: fold_partner names each column once, and the partner of column i lies among the columns 128 * (15 - i // 128) to 128 * (16 - i // 128) - 1.
All inputs are finite; a program needn't handle non-finite values. No bound on the sum of `land_mask` or of `ice_mask` on one device may be relied on, other than what follows from the above.
Results may differ from the reference program's by a relative error of at most 0.00014.
Values sent between devices are 32-bit elements; how exact they have to be, the bound alone decides.
A program may use at most 64 MiB of HBM per device.

```python
import math
import jax
import jax.numpy as jnp

CX = 128
EVP_ITERS = 4
SUBSTEPS = 6
NY = 3584
NX = 2048


def draw_fold_partner(key, part):
    block_count = NX // CX
    block_ids = jnp.arange(block_count, dtype=jnp.int32)

    def shuffle_block(block_id):
        return jax.random.permutation(jax.random.fold_in(key, block_id), CX).astype(jnp.int32)
    shuffles = jax.vmap(shuffle_block)(block_ids)
    mirrored = (block_count - 1 - block_ids)[:, None] * CX + shuffles
    return mirrored.reshape(NX).astype(jnp.int32)


def touch_ends(values, stream_key, least, top_value):
    longest = values.shape.index(max(values.shape))
    spots = []
    for shift in (0, 1):
        where = [jax.random.randint(jax.random.fold_in(stream_key, axis), (), 0, length) for axis, length in enumerate(values.shape)]
        where[longest] = (where[longest] + shift) % values.shape[longest]
        spots.append(tuple(where))
    return values.at[spots[0]].set(least).at[spots[1]].set(top_value)


def levels(stream_key, dims, cuts, low, top_value):
    def one(dim, blocks):
        heights = jax.random.uniform(jax.random.fold_in(jax.random.fold_in(stream_key, 6), dim), (blocks,), jnp.float32, low / len(cuts), top_value / len(cuts))
        return jnp.repeat(jnp.exp(heights), dims[dim] // blocks).reshape((-1,) + (1,) * (len(dims) - dim - 1))

    loudness = one(*cuts[0])
    for cut in cuts[1:]:
        loudness = loudness * one(*cut)
    return loudness


def scatter_about(key, dims, scale, reach, cuts=(), held_as=jnp.bfloat16):
    entries = scale * jax.random.normal(key, dims, jnp.float32)
    if cuts:
        entries = entries * levels(key, dims, cuts, -0.22, 0.18)
    return jnp.clip(entries, -reach, reach).astype(held_as)


def setup_inputs(seed: int = 0) -> dict:
    keys = jax.random.split(jax.random.key(seed), 12)
    return {
        "ice_velocity": scatter_about(keys[0], (2, NY, NX), 1.0, 6.0, ((1, 16), (2, 16)), jnp.float32),
        "ice_stress": scatter_about(keys[1], (3, NY, NX), 0.5, 3.0, ((1, 16), (2, 16)), jnp.float32),
        "ice_mass": jnp.clip(jnp.exp(math.log(4.0) - 2.0794415 * jax.random.uniform(keys[2], (NY, NX), jnp.float32) ** levels(keys[2], (NY, NX), ((0, 16), (1, 16)), -0.2, 0.2)), 0.5, 4.0),
        "ice_strength": jnp.clip(jnp.exp(math.log(4.0) - 2.0794415 * jax.random.uniform(keys[3], (NY, NX), jnp.float32) ** levels(keys[3], (NY, NX), ((0, 16), (1, 16)), -0.2, 0.2)), 0.5, 4.0),
        "wind_stress": scatter_about(keys[4], (2, NY, NX), 0.5, 3.0, ((1, 16), (2, 16)), jnp.float32),
        "sea_level": scatter_about(keys[5], (NY, NX), 0.5, 3.0, ((0, 16), (1, 16)), jnp.float32),
        "transport": scatter_about(keys[6], (2, NY, NX), 1.0, 6.0, ((1, 16), (2, 16)), jnp.float32),
        "depth": jnp.clip(jnp.exp(math.log(2.0) - 1.3862944 * jax.random.uniform(keys[7], (NY, NX), jnp.float32) ** levels(keys[7], (NY, NX), ((0, 16), (1, 16)), -0.2, 0.2)), 0.5, 2.0),
        "land_mask": touch_ends((jax.random.randint(keys[8], (NY, NX), 0, 10) < 9).astype(jnp.int32), jax.random.fold_in(keys[8], 1), 0, 1),
        "ice_mask": touch_ends((jax.random.randint(keys[9], (NY, NX), 0, 3) < 2).astype(jnp.int32), jax.random.fold_in(keys[9], 1), 0, 1),
        "fold_partner": draw_fold_partner(jax.random.fold_in(keys[11], 71), 0),
    }


DT_ICE = 1.0
DT_SEA = 0.5
CDW = 0.5
ALPHA_MIN = 2.0
ALPHA_C = 16.0
INV_E2 = 0.25
DMIN = 0.05
FCOR = 0.5
GRAV = 1.0
RBOT = 0.2

def centre_x(field):
    return (field[..., 1:-1, 2:] - field[..., 1:-1, :-2]) * 0.5

def centre_y(field):
    return (field[..., 2:, 1:-1] - field[..., :-2, 1:-1]) * 0.5

def interior(field):
    return field[..., 1:-1, 1:-1]

def latitude_factor(row_index, total_rows):
    angle_rows = jnp.pi * ((row_index.astype(jnp.float32) + 0.5) / total_rows - 0.5)
    return (FCOR * jnp.sin(angle_rows))[:, None]

def rheology(extended, statics, start_velocity, ocean_velocity, wind_stress, coriolis):
    ice_u = extended[0, 2:-2, 2:-2]
    ice_v = extended[1, 2:-2, 2:-2]
    strain_xx = centre_x(extended[0])
    strain_yy = centre_y(extended[1])
    shear_rate = centre_y(extended[0]) + centre_x(extended[1])
    divergence = strain_xx + strain_yy
    tension = strain_xx - strain_yy
    deformation = jnp.sqrt(divergence * divergence + (tension * tension + shear_rate * shear_rate) * INV_E2 + DMIN * DMIN)
    strength = interior(statics[0])
    ice_cover = interior(statics[2] * statics[3])
    mass_rim = interior(statics[1]) + 1.0 - ice_cover
    relaxation = ALPHA_MIN + jnp.sqrt(ALPHA_C * strength / mass_rim)
    stress_sum = ice_cover * (relaxation * interior(extended[2]) + strength * (divergence / deformation - 1.0)) / (1.0 + relaxation)
    stress_diff = ice_cover * (relaxation * interior(extended[3]) + strength * tension * INV_E2 / deformation) / (1.0 + relaxation)
    stress_xy = ice_cover * (relaxation * interior(extended[4]) + strength * shear_rate * (0.5 * INV_E2) / deformation) / (1.0 + relaxation)
    stress_xx = 0.5 * (stress_sum + stress_diff)
    stress_yy = 0.5 * (stress_sum - stress_diff)
    force_x = centre_x(stress_xx) + centre_y(stress_xy)
    force_y = centre_x(stress_xy) + centre_y(stress_yy)
    inertia = interior(relaxation)
    mass_cell = interior(mass_rim)
    cover_cell = interior(ice_cover)
    rel_x = ocean_velocity[0] - ice_u
    rel_y = ocean_velocity[1] - ice_v
    drag_coef = CDW * jnp.sqrt(rel_x * rel_x + rel_y * rel_y)
    denominator = 1.0 + inertia + DT_ICE * drag_coef / mass_cell
    new_u = cover_cell * (inertia * ice_u + start_velocity[0] + DT_ICE / mass_cell * (force_x + wind_stress[0] + drag_coef * ocean_velocity[0]) + DT_ICE * coriolis * ice_v) / denominator
    new_v = cover_cell * (inertia * ice_v + start_velocity[1] + DT_ICE / mass_cell * (force_y + wind_stress[1] + drag_coef * ocean_velocity[1]) - DT_ICE * coriolis * ice_u) / denominator
    return jnp.stack([new_u, new_v, interior(stress_sum), interior(stress_diff), interior(stress_xy)])

def barotropic(extended, land_rim, depth, surface_stress, coriolis):
    new_level = interior(land_rim) * (interior(extended[0]) - DT_SEA * (centre_x(extended[1]) + centre_y(extended[2])))
    flow_x = extended[1, 2:-2, 2:-2]
    flow_y = extended[2, 2:-2, 2:-2]
    land_cell = land_rim[2:-2, 2:-2]
    damping = 1.0 + DT_SEA * RBOT / depth
    next_x = land_cell * (flow_x - DT_SEA * (GRAV * depth * centre_x(new_level) - coriolis * flow_y - surface_stress[0])) / damping
    next_y = land_cell * (flow_y - DT_SEA * (GRAV * depth * centre_y(new_level) + coriolis * flow_x - surface_stress[1])) / damping
    return jnp.stack([interior(new_level), next_x, next_y])

def reference(ice_velocity, ice_stress, ice_mass, ice_strength, wind_stress, sea_level, transport, depth, land_mask, ice_mask, fold_partner):

    def extend(field_stack, sign_list):
        flipped = jnp.flip(field_stack[:, -2:, :], axis=1)
        fold_part = jnp.take(flipped, fold_partner, axis=2) * sign_list[:, None, None]
        south_part = jnp.zeros_like(flipped)
        column_set = jnp.concatenate([south_part, field_stack, fold_part], axis=1)
        return jnp.concatenate([column_set[:, :, -2:], column_set, column_set[:, :, :2]], axis=2)
    total_rows = sea_level.shape[0]
    coriolis = latitude_factor(jnp.arange(total_rows, dtype=jnp.int32), total_rows)
    ocean_velocity = transport / depth[None]
    static_signs = jnp.array([1.0, 1.0, 1.0, 1.0], jnp.float32)
    ice_signs = jnp.array([-1.0, -1.0, 1.0, 1.0, 1.0], jnp.float32)
    sea_signs = jnp.array([1.0, -1.0, -1.0], jnp.float32)
    statics = extend(jnp.stack([ice_strength, ice_mass, land_mask.astype(jnp.float32), ice_mask.astype(jnp.float32)]), static_signs)
    ice_state = jnp.concatenate([ice_velocity, ice_stress], axis=0)
    for iteration in range(EVP_ITERS):
        ice_state = rheology(extend(ice_state, ice_signs), statics, ice_velocity, ocean_velocity, wind_stress, coriolis)
    final_velocity = ice_state[:2]
    cover_cell = statics[2, 2:-2, 2:-2] * statics[3, 2:-2, 2:-2]
    rel_x = final_velocity[0] - ocean_velocity[0]
    rel_y = final_velocity[1] - ocean_velocity[1]
    drag_coef = CDW * jnp.sqrt(rel_x * rel_x + rel_y * rel_y)
    surface_stress = cover_cell * drag_coef * (final_velocity - ocean_velocity) + (1.0 - cover_cell) * wind_stress
    sea_state = jnp.concatenate([sea_level[None], transport], axis=0)
    for substep in range(SUBSTEPS):
        sea_state = barotropic(extend(sea_state, sea_signs), statics[2], depth, surface_stress, coriolis)
    return (final_velocity, ice_state[2:], sea_state[0], sea_state[1:])
```

```python
import math

import jax
import jax.numpy as jnp
from jax import lax
from jax.experimental import pallas as pl
from jax.experimental.pallas import tpu as pltpu
from jax.sharding import PartitionSpec as P

ICE_GROUPS = (2, 2)
SEA_GROUPS = (3, 3)
EDGE = 16
ICE_CHUNK = 24
SEA_CHUNK = 24
LANES = 128
MESH_ID = pl.DeviceIdType.MESH

U, V, S1, S2, S12, STRENGTH, MASSX, COVER, WX, WY, OU, OV = range(12)
C1, C2, RELAX, INVM, KU, KV = range(6)
LEVEL, TU, TV, DEPTH, LAND, SX, SY = range(7)
ICE_SIGNS = {U: -1.0, V: -1.0}
SEA_SIGNS = {TU: -1.0, TV: -1.0}


class Exchange:
    def __init__(self, name, fields, steps, rows):
        self.name, self.fields, self.steps = name, fields, steps
        self.width = 2 * steps
        self.groups = 4 if len(fields) * self.width <= 32 else 2
        self.group_lanes = LANES // self.groups
        assert len(fields) * self.width <= self.group_lanes
        self.group_rows = rows // self.groups
        self.extra = name == "ice0"
        count = len(fields) * self.width + (1 if self.extra else 0)
        self.strip_rows = -(-count // 8) * 8

    def scratch(self, blocks):
        f32 = jnp.float32
        packed, got = (self.group_rows, LANES), (self.group_rows + 16, LANES)
        strip = (self.strip_rows, LANES)
        return dict(
            top=pltpu.VMEM(strip, f32),
            bot=pltpu.VMEM(strip, f32),
            low=pltpu.VMEM(strip, f32),
            high=pltpu.VMEM(strip, f32),
            west=pltpu.VMEM(packed, f32),
            east=pltpu.VMEM(packed, f32),
            right=pltpu.VMEM(got, f32),
            left=pltpu.VMEM(got, f32),
            strips=pltpu.VMEM((blocks * self.strip_rows, LANES), f32),
            send=pltpu.SemaphoreType.DMA((8,)),
            recv=pltpu.SemaphoreType.DMA((8,)),
            strip_send=pltpu.SemaphoreType.DMA((blocks,)),
            strip_recv=pltpu.SemaphoreType.DMA((blocks,)),
        )


def plan(rows):
    ice = [Exchange(f"ice{i}", list(range(12 if i == 0 else 5)), s, rows) for i, s in enumerate(ICE_GROUPS)]
    first = Exchange("sea0", [LEVEL, TU, TV, DEPTH, LAND], SEA_GROUPS[0], rows)
    surf = Exchange("surf", [SX, SY], SEA_GROUPS[0], rows)
    later = [Exchange(f"sea{i}", [LEVEL, TU, TV], s, rows) for i, s in enumerate(SEA_GROUPS) if i]
    return ice, first, surf, later


def kernel_body(
    blocks,
    bands,
    names,
    vel_in,
    str_in,
    mass_in,
    strength_in,
    wind_in,
    level_in,
    trans_in,
    depth_in,
    land_in,
    icemask_in,
    partner_in,
    vel_out,
    str_out,
    level_out,
    trans_out,
    *scratch,
):
    ref = dict(zip(names, scratch))
    ice, der, sea, cor = ref["ice"], ref["der"], ref["sea"], ref["cor"]
    ist, ider, sst, sder = ref["ist"], ref["ider"], ref["sst"], ref["sder"]
    masks, partner, perm = ref["masks"], ref["partner"], ref["perm"]
    in_sem, out_sem = ref["in_sem"], ref["out_sem"]
    rows = mass_in.shape[0]
    total_rows = rows * bands
    own = slice(EDGE, EDGE + rows)
    full = rows + 16
    gy, gx = lax.axis_index("gy"), lax.axis_index("gx")
    west_x, east_x = lax.rem(gx + blocks - 1, blocks), lax.rem(gx + 1, blocks)
    is_top, is_low = gy == bands - 1, gy == 0
    ice_ex, sea_ex, surf_ex, later_ex = plan(rows)

    barrier = pltpu.get_barrier_semaphore()

    def greet(y, x):
        pl.semaphore_signal(barrier, inc=1, device_id=(y, x), device_id_type=MESH_ID)

    greet(gy, west_x)
    greet(gy, east_x)

    @pl.when(gy < bands - 1)
    def _():
        for x in (gx, west_x, east_x):
            greet(gy + 1, x)

    @pl.when(gy > 0)
    def _():
        for x in (gx, west_x, east_x):
            greet(gy - 1, x)

    @pl.when(is_top)
    def _():
        def one(j, carry):
            greet(gy, lax.rem(gx + j, blocks))
            return carry

        lax.fori_loop(1, blocks, one, 0)

    loads = [
        (vel_in, ice.at[U : V + 1, 0, own]),
        (str_in, ice.at[S1 : S12 + 1, 0, own]),
        (mass_in, ice.at[MASSX, 0, own]),
        (strength_in, ice.at[STRENGTH, 0, own]),
        (wind_in, ice.at[WX : WY + 1, 0, own]),
        (level_in, sea.at[LEVEL, 0, own]),
        (trans_in, sea.at[TU : TV + 1, 0, own]),
        (depth_in, sea.at[DEPTH, 0, own]),
        (land_in, masks.at[0]),
        (icemask_in, masks.at[1]),
        (partner_in, partner),
    ]
    loads = [pltpu.make_async_copy(a, b, in_sem.at[i]) for i, (a, b) in enumerate(loads)]
    for copy in loads:
        copy.start()

    def loop(count, body):
        def one(i, carry):
            body(i)
            return carry

        lax.fori_loop(0, count, one, 0)

    def coriolis(i):
        at = pl.multiple_of(i * 8, 8)
        r = lax.broadcasted_iota(jnp.int32, (8, LANES), 0) + (gy * rows + at - EDGE)
        angle = jnp.pi * ((r.astype(jnp.float32) + 0.5) / total_rows - 0.5)
        cor[pl.ds(at, 8), :] = 0.5 * jnp.sin(angle)

    loop((rows + 2 * EDGE) // 8, coriolis)
    for copy in loads:
        copy.wait()

    def prepare(i):
        at = pl.multiple_of(i * 8, 8)
        here, m = pl.ds(at + EDGE, 8), pl.ds(at, 8)
        land = masks[0, m, :].astype(jnp.float32)
        cover = land * masks[1, m, :].astype(jnp.float32)
        depth = sea[DEPTH, 0, here, :]
        sea[LAND, 0, here, :] = land
        ice[COVER, 0, here, :] = cover
        ice[MASSX, 0, here, :] = ice[MASSX, 0, here, :] + 1.0 - cover
        ice[OU, 0, here, :] = sea[TU, 0, here, :] / depth
        ice[OV, 0, here, :] = sea[TV, 0, here, :] / depth

    loop(rows // 8, prepare)

    lane8 = lax.broadcasted_iota(jnp.int32, (8, LANES), 1)

    def stage(ex, store):
        w = ex.width
        top, bot = ref[ex.name, "top"], ref[ex.name, "bot"]
        for k, f in enumerate(ex.fields):
            top[k * w : (k + 1) * w, :] = store[f, 0, EDGE + rows - w : EDGE + rows, :]
            bot[k * w : (k + 1) * w, :] = store[f, 0, EDGE : EDGE + w, :]
        if ex.extra:
            at = len(ex.fields) * w
            local = partner[...] - (blocks - 1 - gx) * LANES
            top[at : at + 1, :] = local.astype(jnp.float32)

        def pack(i):
            to_west = to_east = None
            for g in range(ex.groups):
                for k, f in enumerate(ex.fields):
                    at = g * ex.group_lanes + k * w
                    here = pl.ds(pl.multiple_of(EDGE + g * ex.group_rows + i * 8, 8), 8)
                    x = store[f, 0, here, :]
                    a = pltpu.roll(x, at, 1) if at else x
                    b = pltpu.roll(x, (at + w) % LANES, 1) if (at + w) % LANES else x
                    if to_west is None:
                        to_west, to_east = a, b
                    else:
                        keep = lane8 < at
                        to_west = jnp.where(keep, to_west, a)
                        to_east = jnp.where(keep, to_east, b)
            m = pl.ds(pl.multiple_of(i * 8, 8), 8)
            ref[ex.name, "west"][m, :] = to_west
            ref[ex.name, "east"][m, :] = to_east

        loop(ex.group_rows // 8, pack)

    def sends(ex):
        r = lambda part: ref[ex.name, part]
        n = ex.group_rows
        last, first = pl.ds(n - 8, 8), pl.ds(0, 8)
        mid, low, high = pl.ds(0, n), pl.ds(n, 8), pl.ds(n + 8, 8)
        up, down, flat = 1, -1, 0
        table = [
            (r("top"), r("low"), up, gx),
            (r("bot"), r("high"), down, gx),
            (r("west"), r("right").at[mid], flat, west_x),
            (r("east"), r("left").at[mid], flat, east_x),
            (r("west").at[last], r("right").at[low], up, west_x),
            (r("east").at[last], r("left").at[low], up, east_x),
            (r("west").at[first], r("right").at[high], down, west_x),
            (r("east").at[first], r("left").at[high], down, east_x),
        ]
        out = []
        for i, (src, dst, dy, x) in enumerate(table):
            copy = pltpu.make_async_remote_copy(
                src_ref=src,
                dst_ref=dst,
                send_sem=r("send").at[i],
                recv_sem=r("recv").at[i],
                device_id=(gy + dy, x),
                device_id_type=MESH_ID,
            )
            out.append((dy, copy))
        return out

    def strip_copy(ex, target, source):
        n = ex.strip_rows
        return pltpu.make_async_remote_copy(
            src_ref=ref[ex.name, "top"],
            dst_ref=ref[ex.name, "strips"].at[pl.ds(pl.multiple_of(source * n, 8), n)],
            send_sem=ref[ex.name, "strip_send"].at[target],
            recv_sem=ref[ex.name, "strip_recv"].at[source],
            device_id=(gy, target),
            device_id_type=MESH_ID,
        )

    def each_strip(ex, action):
        reach = ex.steps

        @pl.when(is_top)
        def _():
            def one(j, carry):
                x = lax.rem(gx + j, blocks)
                gap = lax.rem(x + gx + 1, blocks)
                near = (j <= reach) | (j >= blocks - reach) | (gap <= reach) | (gap >= blocks - reach)

                @pl.when(near)
                def _():
                    action(x)

                return carry

            lax.fori_loop(1, blocks, one, 0)

    def start(ex):
        each_strip(ex, lambda x: strip_copy(ex, x, gx).start())
        copies = sends(ex)
        for dy in (0, 1, -1):
            chosen = [c for d, c in copies if d == dy]

            def go(chosen=chosen):
                for c in chosen:
                    c.start()

            if dy == 0:
                go()
            else:
                pl.when((gy < bands - 1) if dy > 0 else (gy > 0))(go)
        n = ex.strip_rows

        @pl.when(is_top)
        def _():
            ref[ex.name, "strips"][pl.ds(pl.multiple_of(gx * n, 8), n), :] = ref[ex.name, "top"][...]

    def wait_recv(ex):
        copies = sends(ex)
        for dy in (0, 1, -1):
            chosen = [c for d, c in copies if d == dy]

            def go(chosen=chosen):
                for c in chosen:
                    c.wait_recv()

            if dy == 0:
                go()
            else:
                pl.when((gy > 0) if dy > 0 else (gy < bands - 1))(go)

    def wait_strips(ex):
        each_strip(ex, lambda x: strip_copy(ex, gx, x).wait_recv())

    def wait_send(ex):
        copies = sends(ex)
        for dy in (0, 1, -1):
            chosen = [c for d, c in copies if d == dy]

            def go(chosen=chosen):
                for c in chosen:
                    c.wait_send()

            if dy == 0:
                go()
            else:
                pl.when((gy < bands - 1) if dy > 0 else (gy > 0))(go)
        each_strip(ex, lambda x: strip_copy(ex, x, gx).wait_send())

    def unpack(ex, store, ones):
        w, n = ex.width, ex.group_rows
        right, left = ref[ex.name, "right"], ref[ex.name, "left"]

        def place(source, g, target):
            x, y = right[source, :], left[source, :]
            for k, f in enumerate(ex.fields):
                at = g * ex.group_lanes + k * w
                a = pltpu.roll(x, (LANES - at) % LANES, 1) if at else x
                shift = (2 * LANES - w - at) % LANES
                b = pltpu.roll(y, shift, 1) if shift else y
                store[f, 1, target, :] = jnp.where(lane8 < LANES // 2, a, b)

        def main(i):
            source = pl.ds(pl.multiple_of(i * 8, 8), 8)
            for g in range(ex.groups):
                place(source, g, pl.ds(pl.multiple_of(EDGE + g * n + i * 8, 8), 8))

        loop(n // 8, main)

        @pl.when(gy > 0)
        def _():
            place(pl.ds(n, 8), ex.groups - 1, pl.ds(EDGE - 8, 8))
            for k, f in enumerate(ex.fields):
                store[f, 0, EDGE - w : EDGE, :] = ref[ex.name, "low"][k * w : (k + 1) * w, :]

        @pl.when(gy < bands - 1)
        def _():
            place(pl.ds(n + 8, 8), 0, pl.ds(EDGE + rows, 8))
            for k, f in enumerate(ex.fields):
                store[f, 0, EDGE + rows : EDGE + rows + w, :] = ref[ex.name, "high"][k * w : (k + 1) * w, :]

        @pl.when(is_low)
        def _():
            for f in ex.fields:
                fill = jnp.full((8, LANES), 1.0 if f == ones else 0.0, jnp.float32)
                store[f, 0, EDGE - 8 : EDGE, :] = fill
                store[f, 1, EDGE - 8 : EDGE, :] = fill

    blane = lax.broadcasted_iota(jnp.int32, (blocks, LANES), 1)
    turn = 7 - lax.broadcasted_iota(jnp.int32, (8, LANES), 0)

    def strip_load(ex, strip):
        w, n = ex.width, ex.strip_rows
        got = ref[ex.name, "strips"]
        for k, f in enumerate(ex.fields):
            for d in range(w):
                strip[f, 2 + d] = got[pl.ds(k * w + w - 1 - d, blocks, stride=n), :]
        if ex.extra:
            perm[...] = got[pl.ds(len(ex.fields) * w, blocks, stride=n), :].astype(jnp.int32)

    def fold_rows(x):
        parts = [jnp.take_along_axis(x[b : b + 8], turn, axis=0) for b in range(blocks - 8, -1, -8)]
        index = perm[...]
        parts = [jnp.take_along_axis(p, index[8 * i : 8 * i + 8], axis=1) for i, p in enumerate(parts)]
        return jnp.concatenate(parts, axis=0)

    def fold(strip, store, fields, signs):
        for f in fields:
            for k in (0, 1):
                x = fold_rows(strip[f, 2 + k])
                strip[f, 1 - k] = -x if f in signs else x
        lane1 = lax.broadcasted_iota(jnp.int32, (1, LANES), 1)
        for f in fields:
            for k in (0, 1):
                row = slice(EDGE + rows + k, EDGE + rows + k + 1)
                store[f, 0, row, :] = strip[f, 1 - k, pl.ds(gx, 1), :]
                store[f, 1, row, :] = jnp.where(
                    lane1 < LANES // 2, strip[f, 1 - k, pl.ds(east_x, 1), :], strip[f, 1 - k, pl.ds(west_x, 1), :]
                )

    def dx_strip(x):
        a = jnp.where(blane == 0, pltpu.roll(x, blocks - 1, 0), x)
        b = jnp.where(blane == LANES - 1, pltpu.roll(x, 1, 0), x)
        return pltpu.roll(a, LANES - 1, 1) - pltpu.roll(b, 1, 1)

    def row_coriolis(i):
        row = total_rows + 1 - i
        return 0.5 * math.sin(math.pi * ((row + 0.5) / total_rows - 0.5))

    def ice_coefficients(strength, massx, cover, u, v, wx, wy):
        relax = 2.0 + jnp.sqrt(16.0 * strength / massx)
        share = cover / (1.0 + relax)
        inv = 1.0 / massx
        return share * relax, share * strength, relax, inv, u + wx * inv, v + wy * inv

    def stresses(exx, eyy, shear, c1, c2, s1, s2, s12):
        div, ten = exx + eyy, exx - eyy
        r = lax.rsqrt(div * div + (ten * ten + shear * shear) * 0.25 + 0.01)
        g = c2 * r
        return c1 * s1 + (g * div - c2), c1 * s2 + (0.25 * g) * ten, c1 * s12 + (0.125 * g) * shear

    def velocities(fx, fy, u, v, relax, inv, cover, ku, kv, ou, ov, f):
        rx, ry = ou - u, ov - v
        drag = 0.5 * jnp.sqrt(rx * rx + ry * ry)
        part = cover / (1.0 + relax + drag * inv)
        new_u = part * (relax * u + ku + inv * (fx + drag * ou) + f * v)
        new_v = part * (relax * v + kv + inv * (fy + drag * ov) - f * u)
        return new_u, new_v

    def dx_pair(m, h, first, last):
        am, ah = jnp.where(first, h, m), jnp.where(first, m, h)
        bm, bh = jnp.where(last, h, m), jnp.where(last, m, h)
        return (
            pltpu.roll(am, LANES - 1, 1) - pltpu.roll(bm, 1, 1),
            pltpu.roll(ah, LANES - 1, 1) - pltpu.roll(bh, 1, 1),
        )

    def ends(chunk):
        lane = lax.broadcasted_iota(jnp.int32, (chunk, LANES), 1)
        return lane == 0, lane == LANES - 1

    def ice_static(i):
        here = pl.ds(pl.multiple_of(EDGE - 8 + i * 8, 8), 8)
        for p in (0, 1):
            got = ice_coefficients(*(ice[f, p, here, :] for f in (STRENGTH, MASSX, COVER, U, V, WX, WY)))
            for f, x in enumerate(got):
                der[f, p, here, :] = x

    def ice_step():
        n = ICE_CHUNK
        first, last = ends(n)

        def stress(i):
            at = pl.multiple_of(EDGE - 8 + i * n, 8)
            here, north, south = pl.ds(at, n), pl.ds(at + 1, n), pl.ds(at - 1, n)
            exx = dx_pair(ice[U, 0, here, :], ice[U, 1, here, :], first, last)
            exv = dx_pair(ice[V, 0, here, :], ice[V, 1, here, :], first, last)
            for p in (0, 1):
                eyy = ice[V, p, north, :] - ice[V, p, south, :]
                shear = ice[U, p, north, :] - ice[U, p, south, :] + exv[p]
                got = stresses(
                    exx[p], eyy, shear, der[C1, p, here, :], der[C2, p, here, :], *(ice[f, p, here, :] for f in (S1, S2, S12))
                )
                for f, x in zip((S1, S2, S12), got):
                    ice[f, p, here, :] = x

        loop(full // n, stress)

        def velocity(i):
            at = pl.multiple_of(EDGE - 8 + i * n, 8)
            here, north, south = pl.ds(at, n), pl.ds(at + 1, n), pl.ds(at - 1, n)
            sums = [ice[S1, p, here, :] + ice[S2, p, here, :] for p in (0, 1)]
            dsum = dx_pair(sums[0], sums[1], first, last)
            dxy = dx_pair(ice[S12, 0, here, :], ice[S12, 1, here, :], first, last)
            f = cor[here, :]
            for p in (0, 1):
                fx = 0.25 * dsum[p] + 0.5 * (ice[S12, p, north, :] - ice[S12, p, south, :])
                dyy = (ice[S1, p, north, :] - ice[S2, p, north, :]) - (ice[S1, p, south, :] - ice[S2, p, south, :])
                fy = 0.5 * dxy[p] + 0.25 * dyy
                u, v = ice[U, p, here, :], ice[V, p, here, :]
                new_u, new_v = velocities(
                    fx,
                    fy,
                    u,
                    v,
                    der[RELAX, p, here, :],
                    der[INVM, p, here, :],
                    ice[COVER, p, here, :],
                    der[KU, p, here, :],
                    der[KV, p, here, :],
                    ice[OU, p, here, :],
                    ice[OV, p, here, :],
                    f,
                )
                ice[U, p, here, :] = new_u
                ice[V, p, here, :] = new_v

        loop(full // n, velocity)

    def ice_strip_static(w):
        for i in range(1, w + 2):
            fields = (STRENGTH, MASSX, COVER, U, V, WX, WY)
            got = ice_coefficients(*(ist[f, i] for f in fields))
            for f, x in enumerate(got):
                ider[f, i] = x

    def ice_strip_step(n):
        for i in range(1, n + 1):
            exx, exv = dx_strip(ist[U, i]), dx_strip(ist[V, i])
            eyy = ist[V, i - 1] - ist[V, i + 1]
            shear = ist[U, i - 1] - ist[U, i + 1] + exv
            got = stresses(exx, eyy, shear, ider[C1, i], ider[C2, i], *(ist[f, i] for f in (S1, S2, S12)))
            for f, x in zip((S1, S2, S12), got):
                ist[f, i] = x
        for i in range(2, n):
            fx = 0.25 * dx_strip(ist[S1, i] + ist[S2, i]) + 0.5 * (ist[S12, i - 1] - ist[S12, i + 1])
            dyy = (ist[S1, i - 1] - ist[S2, i - 1]) - (ist[S1, i + 1] - ist[S2, i + 1])
            fy = 0.5 * dx_strip(ist[S12, i]) + 0.25 * dyy
            new_u, new_v = velocities(
                fx,
                fy,
                ist[U, i],
                ist[V, i],
                ider[RELAX, i],
                ider[INVM, i],
                ist[COVER, i],
                ider[KU, i],
                ider[KV, i],
                ist[OU, i],
                ist[OV, i],
                row_coriolis(i),
            )
            ist[U, i] = new_u
            ist[V, i] = new_v

    def sea_coefficients(depth, land):
        return land / (1.0 + 0.1 / depth), 0.25 * depth

    def sea_static(i):
        here = pl.ds(pl.multiple_of(EDGE - 8 + i * 8, 8), 8)
        for p in (0, 1):
            a, b = sea_coefficients(sea[DEPTH, p, here, :], sea[LAND, p, here, :])
            der[0, p, here, :] = a
            der[1, p, here, :] = b

    def flows(tu, tv, part, slope, dlx, dly, f, sx, sy):
        east = part * (tu - slope * dlx + (0.5 * f) * tv + 0.5 * sx)
        north = part * (tv - slope * dly - (0.5 * f) * tu + 0.5 * sy)
        return east, north

    def sea_step():
        n = SEA_CHUNK
        first, last = ends(n)

        def level(i):
            at = pl.multiple_of(EDGE - 8 + i * n, 8)
            here, north, south = pl.ds(at, n), pl.ds(at + 1, n), pl.ds(at - 1, n)
            du = dx_pair(sea[TU, 0, here, :], sea[TU, 1, here, :], first, last)
            for p in (0, 1):
                dv = sea[TV, p, north, :] - sea[TV, p, south, :]
                sea[LEVEL, p, here, :] = sea[LAND, p, here, :] * (sea[LEVEL, p, here, :] - 0.25 * (du[p] + dv))

        loop(full // n, level)

        def flow(i):
            at = pl.multiple_of(EDGE - 8 + i * n, 8)
            here, north, south = pl.ds(at, n), pl.ds(at + 1, n), pl.ds(at - 1, n)
            dlx = dx_pair(sea[LEVEL, 0, here, :], sea[LEVEL, 1, here, :], first, last)
            f = cor[here, :]
            for p in (0, 1):
                dly = sea[LEVEL, p, north, :] - sea[LEVEL, p, south, :]
                east, nrth = flows(
                    sea[TU, p, here, :],
                    sea[TV, p, here, :],
                    der[0, p, here, :],
                    der[1, p, here, :],
                    dlx[p],
                    dly,
                    f,
                    sea[SX, p, here, :],
                    sea[SY, p, here, :],
                )
                sea[TU, p, here, :] = east
                sea[TV, p, here, :] = nrth

        loop(full // n, flow)

    def sea_strip_static(w):
        for i in range(2, w + 2):
            a, b = sea_coefficients(sst[DEPTH, i], sst[LAND, i])
            sder[0, i] = a
            sder[1, i] = b

    def sea_strip_step(n):
        for i in range(1, n + 1):
            dv = sst[TV, i - 1] - sst[TV, i + 1]
            sst[LEVEL, i] = sst[LAND, i] * (sst[LEVEL, i] - 0.25 * (dx_strip(sst[TU, i]) + dv))
        for i in range(2, n):
            dly = sst[LEVEL, i - 1] - sst[LEVEL, i + 1]
            east, nrth = flows(
                sst[TU, i],
                sst[TV, i],
                sder[0, i],
                sder[1, i],
                dx_strip(sst[LEVEL, i]),
                dly,
                row_coriolis(i),
                sst[SX, i],
                sst[SY, i],
            )
            sst[TU, i] = east
            sst[TV, i] = nrth

    stage(ice_ex[0], ice)
    greeted = 2 + 3 * (gy < bands - 1).astype(jnp.int32) + 3 * (gy > 0).astype(jnp.int32)
    pl.semaphore_wait(barrier, greeted + (blocks - 1) * is_top.astype(jnp.int32))
    start(ice_ex[0])
    stage(sea_ex, sea)
    start(sea_ex)

    state = (U, V, S1, S2, S12)
    for number, ex in enumerate(ice_ex):
        if number:
            stage(ex, ice)
            start(ex)
        wait_recv(ex)
        unpack(ex, ice, MASSX)
        wait_strips(ex)

        @pl.when(is_top)
        def _(ex=ex, number=number):
            strip_load(ex, ist)
            fold(ist, ice, state + ((STRENGTH, MASSX, COVER, WX, WY) if number == 0 else ()), ICE_SIGNS)
            if number == 0:
                ice_strip_static(ex.width)

        if number == 0:
            loop(full // 8, ice_static)
        for step in range(ex.steps):
            if step:

                @pl.when(is_top)
                def _(n=ex.width - 2 * (step - 1)):
                    ice_strip_step(n)
                    fold(ist, ice, state, ICE_SIGNS)

            ice_step()

    outs = [
        pltpu.make_async_copy(ice.at[U : V + 1, 0, own], vel_out, out_sem.at[0]),
        pltpu.make_async_copy(ice.at[S1 : S12 + 1, 0, own], str_out, out_sem.at[1]),
    ]

    def surface(i):
        here = pl.ds(pl.multiple_of(EDGE + i * 8, 8), 8)
        cover = ice[COVER, 0, here, :]
        rx, ry = ice[U, 0, here, :] - ice[OU, 0, here, :], ice[V, 0, here, :] - ice[OV, 0, here, :]
        drag = cover * (0.5 * jnp.sqrt(rx * rx + ry * ry))
        sea[SX, 0, here, :] = drag * rx + (1.0 - cover) * ice[WX, 0, here, :]
        sea[SY, 0, here, :] = drag * ry + (1.0 - cover) * ice[WY, 0, here, :]

    loop(rows // 8, surface)
    stage(surf_ex, sea)
    start(surf_ex)
    for copy in outs:
        copy.start()
    flow_state = (LEVEL, TU, TV)
    for number, ex in enumerate([sea_ex] + later_ex):
        if number:
            stage(ex, sea)
            start(ex)
        wait_recv(ex)
        unpack(ex, sea, DEPTH)
        wait_strips(ex)

        @pl.when(is_top)
        def _(ex=ex, number=number):
            strip_load(ex, sst)
            fold(sst, sea, flow_state + ((DEPTH, LAND) if number == 0 else ()), SEA_SIGNS)
            if number == 0:
                sea_strip_static(ex.width)

        if number == 0:
            loop(full // 8, sea_static)
            wait_recv(surf_ex)
            unpack(surf_ex, sea, DEPTH)
            wait_strips(surf_ex)

            @pl.when(is_top)
            def _():
                strip_load(surf_ex, sst)

        for step in range(ex.steps):
            if step:

                @pl.when(is_top)
                def _(n=ex.width - 2 * (step - 1)):
                    sea_strip_step(n)
                    fold(sst, sea, flow_state, SEA_SIGNS)

            sea_step()

    outs += [
        pltpu.make_async_copy(sea.at[LEVEL, 0, own], level_out, out_sem.at[2]),
        pltpu.make_async_copy(sea.at[TU : TV + 1, 0, own], trans_out, out_sem.at[3]),
    ]
    for copy in outs[2:]:
        copy.start()
    for ex in ice_ex + [sea_ex, surf_ex] + later_ex:
        wait_send(ex)
    for copy in outs:
        copy.wait()


def per_device(blocks, bands, *args):
    f32 = jnp.float32
    rows = args[2].shape[0]
    tall = rows + 2 * EDGE
    ice_ex, sea_ex, surf_ex, later_ex = plan(rows)
    depth = 2 + 2 * max(ICE_GROUPS + SEA_GROUPS)
    scratch = dict(
        ice=pltpu.VMEM((12, 2, tall, LANES), f32),
        der=pltpu.VMEM((6, 2, tall, LANES), f32),
        sea=pltpu.VMEM((7, 2, tall, LANES), f32),
        cor=pltpu.VMEM((tall, LANES), f32),
        ist=pltpu.VMEM((12, depth, blocks, LANES), f32),
        ider=pltpu.VMEM((6, depth, blocks, LANES), f32),
        sst=pltpu.VMEM((7, depth, blocks, LANES), f32),
        sder=pltpu.VMEM((2, depth, blocks, LANES), f32),
        masks=pltpu.VMEM((2, rows, LANES), jnp.int32),
        partner=pltpu.VMEM((1, LANES), jnp.int32),
        perm=pltpu.VMEM((blocks, LANES), jnp.int32),
        in_sem=pltpu.SemaphoreType.DMA((11,)),
        out_sem=pltpu.SemaphoreType.DMA((4,)),
    )
    for ex in ice_ex + [sea_ex, surf_ex] + later_ex:
        for part, space in ex.scratch(blocks).items():
            scratch[ex.name, part] = space

    def body(*refs):
        kernel_body(blocks, bands, list(scratch), *refs)

    sds = jax.ShapeDtypeStruct
    args = args[:-1] + (args[-1].reshape(1, LANES),)
    anywhere = pl.BlockSpec(memory_space=pl.ANY)
    return pl.pallas_call(
        body,
        out_shape=(
            sds((2, rows, LANES), f32),
            sds((3, rows, LANES), f32),
            sds((rows, LANES), f32),
            sds((2, rows, LANES), f32),
        ),
        in_specs=[anywhere] * 11,
        out_specs=(anywhere,) * 4,
        scratch_shapes=list(scratch.values()),
        compiler_params=pltpu.CompilerParams(
            collective_id=0, has_side_effects=True, vmem_limit_bytes=67043328
        ),
        name="coupled_step",
    )(*args)


def solution(mesh):
    blocks, bands = mesh.shape["gx"], mesh.shape["gy"]
    flat, stacked = P("gy", "gx"), P(None, "gy", "gx")
    in_specs = (stacked, stacked, flat, flat, stacked, flat, stacked, flat, flat, flat, P("gx"))

    def step(*args):
        return per_device(blocks, bands, *args)

    return jax.shard_map(
        step, mesh=mesh, in_specs=in_specs, out_specs=(stacked, stacked, flat, stacked), check_vma=False
    )
```

```python
import math

import jax
import jax.numpy as jnp
from jax import lax
from jax.experimental import pallas as pl
from jax.experimental.pallas import tpu as pltpu
from jax.sharding import PartitionSpec as P

ICE_GROUPS = (2, 2)
SEA_GROUPS = (3, 3)
EDGE = 16
ICE_CHUNK = 240
SEA_CHUNK = 240
LANES = 128
MESH_ID = pl.DeviceIdType.MESH

U, V, S1, S2, S12, STRENGTH, MASSX, COVER, WX, WY, OU, OV = range(12)
C1, C2, RELAX, INVM, KU, KV = range(6)
LEVEL, TU, TV, DEPTH, LAND, SX, SY = range(7)
ICE_SIGNS = {U: -1.0, V: -1.0}
SEA_SIGNS = {TU: -1.0, TV: -1.0}


class Exchange:
    def __init__(self, name, fields, steps, rows):
        self.name, self.fields, self.steps = name, fields, steps
        self.width = 2 * steps
        self.groups = 4 if len(fields) * self.width <= 32 else 2
        self.group_lanes = LANES // self.groups
        assert len(fields) * self.width <= self.group_lanes
        self.group_rows = rows // self.groups
        self.extra = name == "ice0"
        count = len(fields) * self.width + (1 if self.extra else 0)
        self.strip_rows = -(-count // 8) * 8

    def scratch(self, blocks):
        f32 = jnp.float32
        packed, got = (self.group_rows, LANES), (self.group_rows + 16, LANES)
        strip = (self.strip_rows, LANES)
        return dict(
            top=pltpu.VMEM(strip, f32),
            bot=pltpu.VMEM(strip, f32),
            low=pltpu.VMEM(strip, f32),
            high=pltpu.VMEM(strip, f32),
            west=pltpu.VMEM(packed, f32),
            east=pltpu.VMEM(packed, f32),
            right=pltpu.VMEM(got, f32),
            left=pltpu.VMEM(got, f32),
            strips=pltpu.VMEM((blocks * self.strip_rows, LANES), f32),
            send=pltpu.SemaphoreType.DMA((8,)),
            recv=pltpu.SemaphoreType.DMA((8,)),
            strip_send=pltpu.SemaphoreType.DMA((blocks,)),
            strip_recv=pltpu.SemaphoreType.DMA((blocks,)),
        )


def plan(rows):
    ice = [Exchange(f"ice{i}", list(range(12 if i == 0 else 5)), s, rows) for i, s in enumerate(ICE_GROUPS)]
    first = Exchange("sea0", [LEVEL, TU, TV, DEPTH, LAND], SEA_GROUPS[0], rows)
    surf = Exchange("surf", [SX, SY], SEA_GROUPS[0], rows)
    later = [Exchange(f"sea{i}", [LEVEL, TU, TV], s, rows) for i, s in enumerate(SEA_GROUPS) if i]
    return ice, first, surf, later


def kernel_body(
    blocks,
    bands,
    names,
    vel_in,
    str_in,
    mass_in,
    strength_in,
    wind_in,
    level_in,
    trans_in,
    depth_in,
    land_in,
    icemask_in,
    partner_in,
    vel_out,
    str_out,
    level_out,
    trans_out,
    *scratch,
):
    ref = dict(zip(names, scratch))
    ice, der, sea, cor = ref["ice"], ref["der"], ref["sea"], ref["cor"]
    ist, ider, sst, sder = ref["ist"], ref["ider"], ref["sst"], ref["sder"]
    masks, partner, perm = ref["masks"], ref["partner"], ref["perm"]
    in_sem, out_sem = ref["in_sem"], ref["out_sem"]
    rows = mass_in.shape[0]
    total_rows = rows * bands
    own = slice(EDGE, EDGE + rows)
    full = rows + 16
    gy, gx = lax.axis_index("gy"), lax.axis_index("gx")
    west_x, east_x = lax.rem(gx + blocks - 1, blocks), lax.rem(gx + 1, blocks)
    is_top, is_low = gy == bands - 1, gy == 0
    ice_ex, sea_ex, surf_ex, later_ex = plan(rows)

    barrier = pltpu.get_barrier_semaphore()

    def greet(y, x):
        pl.semaphore_signal(barrier, inc=1, device_id=(y, x), device_id_type=MESH_ID)

    greet(gy, west_x)
    greet(gy, east_x)

    @pl.when(gy < bands - 1)
    def _():
        for x in (gx, west_x, east_x):
            greet(gy + 1, x)

    @pl.when(gy > 0)
    def _():
        for x in (gx, west_x, east_x):
            greet(gy - 1, x)

    @pl.when(is_top)
    def _():
        def one(j, carry):
            greet(gy, lax.rem(gx + j, blocks))
            return carry

        lax.fori_loop(1, blocks, one, 0)

    loads = [
        (vel_in, ice.at[U : V + 1, 0, own]),
        (str_in, ice.at[S1 : S12 + 1, 0, own]),
        (mass_in, ice.at[MASSX, 0, own]),
        (strength_in, ice.at[STRENGTH, 0, own]),
        (wind_in, ice.at[WX : WY + 1, 0, own]),
        (level_in, sea.at[LEVEL, 0, own]),
        (trans_in, sea.at[TU : TV + 1, 0, own]),
        (depth_in, sea.at[DEPTH, 0, own]),
        (land_in, masks.at[0]),
        (icemask_in, masks.at[1]),
        (partner_in, partner),
    ]
    loads = [pltpu.make_async_copy(a, b, in_sem.at[i]) for i, (a, b) in enumerate(loads)]
    for copy in loads:
        copy.start()

    def loop(count, body):
        for i in range(count):
            body(i)

    def coriolis(i):
        at = i * 8
        r = lax.broadcasted_iota(jnp.int32, (8, LANES), 0) + (gy * rows + at - EDGE)
        angle = jnp.pi * ((r.astype(jnp.float32) + 0.5) / total_rows - 0.5)
        cor[pl.ds(at, 8), :] = 0.5 * jnp.sin(angle)

    loop((rows + 2 * EDGE) // 8, coriolis)
    for copy in loads:
        copy.wait()

    def prepare(i):
        at = i * 8
        here, m = pl.ds(at + EDGE, 8), pl.ds(at, 8)
        land = masks[0, m, :].astype(jnp.float32)
        cover = land * masks[1, m, :].astype(jnp.float32)
        depth = sea[DEPTH, 0, here, :]
        sea[LAND, 0, here, :] = land
        ice[COVER, 0, here, :] = cover
        ice[MASSX, 0, here, :] = ice[MASSX, 0, here, :] + 1.0 - cover
        ice[OU, 0, here, :] = sea[TU, 0, here, :] / depth
        ice[OV, 0, here, :] = sea[TV, 0, here, :] / depth

    loop(rows // 8, prepare)

    lane8 = lax.broadcasted_iota(jnp.int32, (8, LANES), 1)

    def stage(ex, store):
        w = ex.width
        top, bot = ref[ex.name, "top"], ref[ex.name, "bot"]
        for k, f in enumerate(ex.fields):
            top[k * w : (k + 1) * w, :] = store[f, 0, EDGE + rows - w : EDGE + rows, :]
            bot[k * w : (k + 1) * w, :] = store[f, 0, EDGE : EDGE + w, :]
        if ex.extra:
            at = len(ex.fields) * w
            local = partner[...] - (blocks - 1 - gx) * LANES
            top[at : at + 1, :] = local.astype(jnp.float32)

        def pack(i):
            to_west = to_east = None
            for g in range(ex.groups):
                for k, f in enumerate(ex.fields):
                    at = g * ex.group_lanes + k * w
                    here = pl.ds(EDGE + g * ex.group_rows + i * 8, 8)
                    x = store[f, 0, here, :]
                    a = pltpu.roll(x, at, 1) if at else x
                    b = pltpu.roll(x, (at + w) % LANES, 1) if (at + w) % LANES else x
                    if to_west is None:
                        to_west, to_east = a, b
                    else:
                        keep = lane8 < at
                        to_west = jnp.where(keep, to_west, a)
                        to_east = jnp.where(keep, to_east, b)
            m = pl.ds(i * 8, 8)
            ref[ex.name, "west"][m, :] = to_west
            ref[ex.name, "east"][m, :] = to_east

        loop(ex.group_rows // 8, pack)

    def sends(ex):
        r = lambda part: ref[ex.name, part]
        n = ex.group_rows
        last, first = pl.ds(n - 8, 8), pl.ds(0, 8)
        mid, low, high = pl.ds(0, n), pl.ds(n, 8), pl.ds(n + 8, 8)
        up, down, flat = 1, -1, 0
        table = [
            (r("top"), r("low"), up, gx),
            (r("bot"), r("high"), down, gx),
            (r("west"), r("right").at[mid], flat, west_x),
            (r("east"), r("left").at[mid], flat, east_x),
            (r("west").at[last], r("right").at[low], up, west_x),
            (r("east").at[last], r("left").at[low], up, east_x),
            (r("west").at[first], r("right").at[high], down, west_x),
            (r("east").at[first], r("left").at[high], down, east_x),
        ]
        out = []
        for i, (src, dst, dy, x) in enumerate(table):
            copy = pltpu.make_async_remote_copy(
                src_ref=src,
                dst_ref=dst,
                send_sem=r("send").at[i],
                recv_sem=r("recv").at[i],
                device_id=(gy + dy, x),
                device_id_type=MESH_ID,
            )
            out.append((dy, copy))
        return out

    def strip_copy(ex, target, source):
        n = ex.strip_rows
        return pltpu.make_async_remote_copy(
            src_ref=ref[ex.name, "top"],
            dst_ref=ref[ex.name, "strips"].at[pl.ds(pl.multiple_of(source * n, 8), n)],
            send_sem=ref[ex.name, "strip_send"].at[target],
            recv_sem=ref[ex.name, "strip_recv"].at[source],
            device_id=(gy, target),
            device_id_type=MESH_ID,
        )

    def each_strip(ex, action):
        reach = ex.steps

        @pl.when(is_top)
        def _():
            def one(j, carry):
                x = lax.rem(gx + j, blocks)
                gap = lax.rem(x + gx + 1, blocks)
                near = (j <= reach) | (j >= blocks - reach) | (gap <= reach) | (gap >= blocks - reach)

                @pl.when(near)
                def _():
                    action(x)

                return carry

            lax.fori_loop(1, blocks, one, 0)

    def start(ex):
        each_strip(ex, lambda x: strip_copy(ex, x, gx).start())
        copies = sends(ex)
        for dy in (0, 1, -1):
            chosen = [c for d, c in copies if d == dy]

            def go(chosen=chosen):
                for c in chosen:
                    c.start()

            if dy == 0:
                go()
            else:
                pl.when((gy < bands - 1) if dy > 0 else (gy > 0))(go)
        n = ex.strip_rows

        @pl.when(is_top)
        def _():
            ref[ex.name, "strips"][pl.ds(pl.multiple_of(gx * n, 8), n), :] = ref[ex.name, "top"][...]

    def wait_recv(ex):
        copies = sends(ex)
        for dy in (0, 1, -1):
            chosen = [c for d, c in copies if d == dy]

            def go(chosen=chosen):
                for c in chosen:
                    c.wait_recv()

            if dy == 0:
                go()
            else:
                pl.when((gy > 0) if dy > 0 else (gy < bands - 1))(go)

    def wait_strips(ex):
        each_strip(ex, lambda x: strip_copy(ex, gx, x).wait_recv())

    def wait_send(ex):
        copies = sends(ex)
        for dy in (0, 1, -1):
            chosen = [c for d, c in copies if d == dy]

            def go(chosen=chosen):
                for c in chosen:
                    c.wait_send()

            if dy == 0:
                go()
            else:
                pl.when((gy < bands - 1) if dy > 0 else (gy > 0))(go)
        each_strip(ex, lambda x: strip_copy(ex, x, gx).wait_send())

    def unpack(ex, store, ones):
        w, n = ex.width, ex.group_rows
        right, left = ref[ex.name, "right"], ref[ex.name, "left"]

        def place(source, g, target):
            x, y = right[source, :], left[source, :]
            for k, f in enumerate(ex.fields):
                at = g * ex.group_lanes + k * w
                a = pltpu.roll(x, (LANES - at) % LANES, 1) if at else x
                shift = (2 * LANES - w - at) % LANES
                b = pltpu.roll(y, shift, 1) if shift else y
                store[f, 1, target, :] = jnp.where(lane8 < LANES // 2, a, b)

        def main(i):
            source = pl.ds(i * 8, 8)
            for g in range(ex.groups):
                place(source, g, pl.ds(EDGE + g * n + i * 8, 8))

        loop(n // 8, main)

        @pl.when(gy > 0)
        def _():
            place(pl.ds(n, 8), ex.groups - 1, pl.ds(EDGE - 8, 8))
            for k, f in enumerate(ex.fields):
                store[f, 0, EDGE - w : EDGE, :] = ref[ex.name, "low"][k * w : (k + 1) * w, :]

        @pl.when(gy < bands - 1)
        def _():
            place(pl.ds(n + 8, 8), 0, pl.ds(EDGE + rows, 8))
            for k, f in enumerate(ex.fields):
                store[f, 0, EDGE + rows : EDGE + rows + w, :] = ref[ex.name, "high"][k * w : (k + 1) * w, :]

        @pl.when(is_low)
        def _():
            for f in ex.fields:
                fill = jnp.full((8, LANES), 1.0 if f == ones else 0.0, jnp.float32)
                store[f, 0, EDGE - 8 : EDGE, :] = fill
                store[f, 1, EDGE - 8 : EDGE, :] = fill

    blane = lax.broadcasted_iota(jnp.int32, (blocks, LANES), 1)
    turn = 7 - lax.broadcasted_iota(jnp.int32, (8, LANES), 0)

    def strip_load(ex, strip):
        w, n = ex.width, ex.strip_rows
        got = ref[ex.name, "strips"]
        for k, f in enumerate(ex.fields):
            for d in range(w):
                strip[f, 2 + d] = got[pl.ds(k * w + w - 1 - d, blocks, stride=n), :]
        if ex.extra:
            perm[...] = got[pl.ds(len(ex.fields) * w, blocks, stride=n), :].astype(jnp.int32)

    def fold_rows(x):
        parts = [jnp.take_along_axis(x[b : b + 8], turn, axis=0) for b in range(blocks - 8, -1, -8)]
        index = perm[...]
        parts = [jnp.take_along_axis(p, index[8 * i : 8 * i + 8], axis=1) for i, p in enumerate(parts)]
        return jnp.concatenate(parts, axis=0)

    def fold(strip, store, fields, signs):
        for f in fields:
            for k in (0, 1):
                x = fold_rows(strip[f, 2 + k])
                strip[f, 1 - k] = -x if f in signs else x
        lane1 = lax.broadcasted_iota(jnp.int32, (1, LANES), 1)
        for f in fields:
            for k in (0, 1):
                row = slice(EDGE + rows + k, EDGE + rows + k + 1)
                store[f, 0, row, :] = strip[f, 1 - k, pl.ds(gx, 1), :]
                store[f, 1, row, :] = jnp.where(
                    lane1 < LANES // 2, strip[f, 1 - k, pl.ds(east_x, 1), :], strip[f, 1 - k, pl.ds(west_x, 1), :]
                )

    def dx_strip(x):
        a = jnp.where(blane == 0, pltpu.roll(x, blocks - 1, 0), x)
        b = jnp.where(blane == LANES - 1, pltpu.roll(x, 1, 0), x)
        return pltpu.roll(a, LANES - 1, 1) - pltpu.roll(b, 1, 1)

    def row_coriolis(i):
        row = total_rows + 1 - i
        return 0.5 * math.sin(math.pi * ((row + 0.5) / total_rows - 0.5))

    def ice_coefficients(strength, massx, cover, u, v, wx, wy):
        relax = 2.0 + jnp.sqrt(16.0 * strength / massx)
        share = cover / (1.0 + relax)
        inv = 1.0 / massx
        return share * relax, share * strength, relax, inv, u + wx * inv, v + wy * inv

    def stresses(exx, eyy, shear, c1, c2, s1, s2, s12):
        div, ten = exx + eyy, exx - eyy
        r = lax.rsqrt(div * div + (ten * ten + shear * shear) * 0.25 + 0.01)
        g = c2 * r
        return c1 * s1 + (g * div - c2), c1 * s2 + (0.25 * g) * ten, c1 * s12 + (0.125 * g) * shear

    def velocities(fx, fy, u, v, relax, inv, cover, ku, kv, ou, ov, f):
        rx, ry = ou - u, ov - v
        drag = 0.5 * jnp.sqrt(rx * rx + ry * ry)
        part = cover / (1.0 + relax + drag * inv)
        new_u = part * (relax * u + ku + inv * (fx + drag * ou) + f * v)
        new_v = part * (relax * v + kv + inv * (fy + drag * ov) - f * u)
        return new_u, new_v

    def dx_pair(m, h, first, last):
        am, ah = jnp.where(first, h, m), jnp.where(first, m, h)
        bm, bh = jnp.where(last, h, m), jnp.where(last, m, h)
        return (
            pltpu.roll(am, LANES - 1, 1) - pltpu.roll(bm, 1, 1),
            pltpu.roll(ah, LANES - 1, 1) - pltpu.roll(bh, 1, 1),
        )

    def ends(chunk):
        lane = lax.broadcasted_iota(jnp.int32, (chunk, LANES), 1)
        return lane == 0, lane == LANES - 1

    def ice_static(i):
        here = pl.ds(EDGE - 8 + i * 8, 8)
        for p in (0, 1):
            got = ice_coefficients(*(ice[f, p, here, :] for f in (STRENGTH, MASSX, COVER, U, V, WX, WY)))
            for f, x in enumerate(got):
                der[f, p, here, :] = x

    def ice_step():
        n = ICE_CHUNK
        first, last = ends(n)

        def stress(i):
            at = EDGE - 8 + i * n
            here, north, south = pl.ds(at, n), pl.ds(at + 1, n), pl.ds(at - 1, n)
            exx = dx_pair(ice[U, 0, here, :], ice[U, 1, here, :], first, last)
            exv = dx_pair(ice[V, 0, here, :], ice[V, 1, here, :], first, last)
            for p in (0, 1):
                eyy = ice[V, p, north, :] - ice[V, p, south, :]
                shear = ice[U, p, north, :] - ice[U, p, south, :] + exv[p]
                got = stresses(
                    exx[p], eyy, shear, der[C1, p, here, :], der[C2, p, here, :], *(ice[f, p, here, :] for f in (S1, S2, S12))
                )
                for f, x in zip((S1, S2, S12), got):
                    ice[f, p, here, :] = x

        loop(full // n, stress)

        def velocity(i):
            at = EDGE - 8 + i * n
            here, north, south = pl.ds(at, n), pl.ds(at + 1, n), pl.ds(at - 1, n)
            sums = [ice[S1, p, here, :] + ice[S2, p, here, :] for p in (0, 1)]
            dsum = dx_pair(sums[0], sums[1], first, last)
            dxy = dx_pair(ice[S12, 0, here, :], ice[S12, 1, here, :], first, last)
            f = cor[here, :]
            for p in (0, 1):
                fx = 0.25 * dsum[p] + 0.5 * (ice[S12, p, north, :] - ice[S12, p, south, :])
                dyy = (ice[S1, p, north, :] - ice[S2, p, north, :]) - (ice[S1, p, south, :] - ice[S2, p, south, :])
                fy = 0.5 * dxy[p] + 0.25 * dyy
                u, v = ice[U, p, here, :], ice[V, p, here, :]
                new_u, new_v = velocities(
                    fx,
                    fy,
                    u,
                    v,
                    der[RELAX, p, here, :],
                    der[INVM, p, here, :],
                    ice[COVER, p, here, :],
                    der[KU, p, here, :],
                    der[KV, p, here, :],
                    ice[OU, p, here, :],
                    ice[OV, p, here, :],
                    f,
                )
                ice[U, p, here, :] = new_u
                ice[V, p, here, :] = new_v

        loop(full // n, velocity)

    def ice_strip_static(w):
        for i in range(1, w + 2):
            fields = (STRENGTH, MASSX, COVER, U, V, WX, WY)
            got = ice_coefficients(*(ist[f, i] for f in fields))
            for f, x in enumerate(got):
                ider[f, i] = x

    def ice_strip_step(n):
        for i in range(1, n + 1):
            exx, exv = dx_strip(ist[U, i]), dx_strip(ist[V, i])
            eyy = ist[V, i - 1] - ist[V, i + 1]
            shear = ist[U, i - 1] - ist[U, i + 1] + exv
            got = stresses(exx, eyy, shear, ider[C1, i], ider[C2, i], *(ist[f, i] for f in (S1, S2, S12)))
            for f, x in zip((S1, S2, S12), got):
                ist[f, i] = x
        for i in range(2, n):
            fx = 0.25 * dx_strip(ist[S1, i] + ist[S2, i]) + 0.5 * (ist[S12, i - 1] - ist[S12, i + 1])
            dyy = (ist[S1, i - 1] - ist[S2, i - 1]) - (ist[S1, i + 1] - ist[S2, i + 1])
            fy = 0.5 * dx_strip(ist[S12, i]) + 0.25 * dyy
            new_u, new_v = velocities(
                fx,
                fy,
                ist[U, i],
                ist[V, i],
                ider[RELAX, i],
                ider[INVM, i],
                ist[COVER, i],
                ider[KU, i],
                ider[KV, i],
                ist[OU, i],
                ist[OV, i],
                row_coriolis(i),
            )
            ist[U, i] = new_u
            ist[V, i] = new_v

    def sea_coefficients(depth, land):
        return land / (1.0 + 0.1 / depth), 0.25 * depth

    def sea_static(i):
        here = pl.ds(EDGE - 8 + i * 8, 8)
        for p in (0, 1):
            a, b = sea_coefficients(sea[DEPTH, p, here, :], sea[LAND, p, here, :])
            der[0, p, here, :] = a
            der[1, p, here, :] = b

    def flows(tu, tv, part, slope, dlx, dly, f, sx, sy):
        east = part * (tu - slope * dlx + (0.5 * f) * tv + 0.5 * sx)
        north = part * (tv - slope * dly - (0.5 * f) * tu + 0.5 * sy)
        return east, north

    def sea_step():
        n = SEA_CHUNK
        first, last = ends(n)

        def level(i):
            at = EDGE - 8 + i * n
            here, north, south = pl.ds(at, n), pl.ds(at + 1, n), pl.ds(at - 1, n)
            du = dx_pair(sea[TU, 0, here, :], sea[TU, 1, here, :], first, last)
            for p in (0, 1):
                dv = sea[TV, p, north, :] - sea[TV, p, south, :]
                sea[LEVEL, p, here, :] = sea[LAND, p, here, :] * (sea[LEVEL, p, here, :] - 0.25 * (du[p] + dv))

        loop(full // n, level)

        def flow(i):
            at = EDGE - 8 + i * n
            here, north, south = pl.ds(at, n), pl.ds(at + 1, n), pl.ds(at - 1, n)
            dlx = dx_pair(sea[LEVEL, 0, here, :], sea[LEVEL, 1, here, :], first, last)
            f = cor[here, :]
            for p in (0, 1):
                dly = sea[LEVEL, p, north, :] - sea[LEVEL, p, south, :]
                east, nrth = flows(
                    sea[TU, p, here, :],
                    sea[TV, p, here, :],
                    der[0, p, here, :],
                    der[1, p, here, :],
                    dlx[p],
                    dly,
                    f,
                    sea[SX, p, here, :],
                    sea[SY, p, here, :],
                )
                sea[TU, p, here, :] = east
                sea[TV, p, here, :] = nrth

        loop(full // n, flow)

    def sea_strip_static(w):
        for i in range(2, w + 2):
            a, b = sea_coefficients(sst[DEPTH, i], sst[LAND, i])
            sder[0, i] = a
            sder[1, i] = b

    def sea_strip_step(n):
        for i in range(1, n + 1):
            dv = sst[TV, i - 1] - sst[TV, i + 1]
            sst[LEVEL, i] = sst[LAND, i] * (sst[LEVEL, i] - 0.25 * (dx_strip(sst[TU, i]) + dv))
        for i in range(2, n):
            dly = sst[LEVEL, i - 1] - sst[LEVEL, i + 1]
            east, nrth = flows(
                sst[TU, i],
                sst[TV, i],
                sder[0, i],
                sder[1, i],
                dx_strip(sst[LEVEL, i]),
                dly,
                row_coriolis(i),
                sst[SX, i],
                sst[SY, i],
            )
            sst[TU, i] = east
            sst[TV, i] = nrth

    stage(ice_ex[0], ice)
    greeted = 2 + 3 * (gy < bands - 1).astype(jnp.int32) + 3 * (gy > 0).astype(jnp.int32)
    pl.semaphore_wait(barrier, greeted + (blocks - 1) * is_top.astype(jnp.int32))
    start(ice_ex[0])
    stage(sea_ex, sea)
    start(sea_ex)

    state = (U, V, S1, S2, S12)
    for number, ex in enumerate(ice_ex):
        if number:
            stage(ex, ice)
            start(ex)
        wait_recv(ex)
        unpack(ex, ice, MASSX)
        wait_strips(ex)

        @pl.when(is_top)
        def _(ex=ex, number=number):
            strip_load(ex, ist)
            fold(ist, ice, state + ((STRENGTH, MASSX, COVER, WX, WY) if number == 0 else ()), ICE_SIGNS)
            if number == 0:
                ice_strip_static(ex.width)

        if number == 0:
            loop(full // 8, ice_static)
        for step in range(ex.steps):
            if step:

                @pl.when(is_top)
                def _(n=ex.width - 2 * (step - 1)):
                    ice_strip_step(n)
                    fold(ist, ice, state, ICE_SIGNS)

            ice_step()

    def surface(i):
        here = pl.ds(EDGE + i * 8, 8)
        cover = ice[COVER, 0, here, :]
        rx, ry = ice[U, 0, here, :] - ice[OU, 0, here, :], ice[V, 0, here, :] - ice[OV, 0, here, :]
        drag = cover * (0.5 * jnp.sqrt(rx * rx + ry * ry))
        sea[SX, 0, here, :] = drag * rx + (1.0 - cover) * ice[WX, 0, here, :]
        sea[SY, 0, here, :] = drag * ry + (1.0 - cover) * ice[WY, 0, here, :]

    loop(rows // 8, surface)
    stage(surf_ex, sea)
    start(surf_ex)
    outs = [
        pltpu.make_async_copy(ice.at[U : V + 1, 0, own], vel_out, out_sem.at[0]),
        pltpu.make_async_copy(ice.at[S1 : S12 + 1, 0, own], str_out, out_sem.at[1]),
        pltpu.make_async_copy(sea.at[LEVEL, 0, own], level_out, out_sem.at[2]),
        pltpu.make_async_copy(sea.at[TU : TV + 1, 0, own], trans_out, out_sem.at[3]),
    ]
    for copy in outs[:2]:
        copy.start()
    flow_state = (LEVEL, TU, TV)
    for number, ex in enumerate([sea_ex] + later_ex):
        if number:
            stage(ex, sea)
            start(ex)
        wait_recv(ex)
        unpack(ex, sea, DEPTH)
        wait_strips(ex)

        @pl.when(is_top)
        def _(ex=ex, number=number):
            strip_load(ex, sst)
            fold(sst, sea, flow_state + ((DEPTH, LAND) if number == 0 else ()), SEA_SIGNS)
            if number == 0:
                sea_strip_static(ex.width)

        if number == 0:
            loop(full // 8, sea_static)
            wait_recv(surf_ex)
            unpack(surf_ex, sea, DEPTH)
            wait_strips(surf_ex)

            @pl.when(is_top)
            def _():
                strip_load(surf_ex, sst)

        for step in range(ex.steps):
            if step:

                @pl.when(is_top)
                def _(n=ex.width - 2 * (step - 1)):
                    sea_strip_step(n)
                    fold(sst, sea, flow_state, SEA_SIGNS)

            sea_step()

    for copy in outs[2:]:
        copy.start()
    for ex in ice_ex + [sea_ex, surf_ex] + later_ex:
        wait_send(ex)
    for copy in outs:
        copy.wait()


def write_out(*refs):
    sources, targets, held, sems = refs[:4], refs[4:8], refs[8:12], refs[12]
    pairs = list(zip(sources, held, targets))
    reads = [pltpu.make_async_copy(a, b, sems.at[0, i]) for i, (a, b, _) in enumerate(pairs)]
    writes = [pltpu.make_async_copy(b, c, sems.at[1, i]) for i, (_, b, c) in enumerate(pairs)]
    for copy in reads:
        copy.start()
    for read, write in zip(reads, writes):
        read.wait()
        write.start()
    for copy in writes:
        copy.wait()


def per_device(blocks, bands, *args):
    f32 = jnp.float32
    rows = args[2].shape[0]
    tall = rows + 2 * EDGE
    ice_ex, sea_ex, surf_ex, later_ex = plan(rows)
    depth = 2 + 2 * max(ICE_GROUPS + SEA_GROUPS)
    scratch = dict(
        ice=pltpu.VMEM((12, 2, tall, LANES), f32),
        der=pltpu.VMEM((6, 2, tall, LANES), f32),
        sea=pltpu.VMEM((7, 2, tall, LANES), f32),
        cor=pltpu.VMEM((tall, LANES), f32),
        ist=pltpu.VMEM((12, depth, blocks, LANES), f32),
        ider=pltpu.VMEM((6, depth, blocks, LANES), f32),
        sst=pltpu.VMEM((7, depth, blocks, LANES), f32),
        sder=pltpu.VMEM((2, depth, blocks, LANES), f32),
        masks=pltpu.VMEM((2, rows, LANES), jnp.int32),
        partner=pltpu.VMEM((1, LANES), jnp.int32),
        perm=pltpu.VMEM((blocks, LANES), jnp.int32),
        in_sem=pltpu.SemaphoreType.DMA((11,)),
        out_sem=pltpu.SemaphoreType.DMA((4,)),
    )
    for ex in ice_ex + [sea_ex, surf_ex] + later_ex:
        for part, space in ex.scratch(blocks).items():
            scratch[ex.name, part] = space

    def body(*refs):
        kernel_body(blocks, bands, list(scratch), *refs)

    sds = jax.ShapeDtypeStruct
    args = args[:-1] + (args[-1].reshape(1, LANES),)
    shapes = (
        sds((2, rows, LANES), f32),
        sds((3, rows, LANES), f32),
        sds((rows, LANES), f32),
        sds((2, rows, LANES), f32),
    )
    far = pl.BlockSpec(memory_space=pltpu.HBM)
    results = pl.pallas_call(
        body,
        out_shape=shapes,
        in_specs=[far] * 11,
        out_specs=(far,) * 4,
        scratch_shapes=list(scratch.values()),
        compiler_params=pltpu.CompilerParams(
            collective_id=0, has_side_effects=True, vmem_limit_bytes=67043328
        ),
        name="coupled_step",
    )(*args)
    return pl.pallas_call(
        write_out,
        out_shape=shapes,
        in_specs=[far] * 4,
        out_specs=(far,) * 4,
        scratch_shapes=[pltpu.VMEM(x.shape, f32) for x in shapes] + [pltpu.SemaphoreType.DMA((2, 4))],
        compiler_params=pltpu.CompilerParams(vmem_limit_bytes=67043328),
        name="write_out",
    )(*results)


def solution(mesh):
    blocks, bands = mesh.shape["gx"], mesh.shape["gy"]
    flat, stacked = P("gy", "gx"), P(None, "gy", "gx")
    in_specs = (stacked, stacked, flat, flat, stacked, flat, stacked, flat, flat, flat, P("gx"))

    def step(*args):
        return per_device(blocks, bands, *args)

    return jax.shard_map(
        step, mesh=mesh, in_specs=in_specs, out_specs=(stacked, stacked, flat, stacked), check_vma=False
    )
```

```python
import math

import jax
import jax.numpy as jnp
from jax import lax
from jax.experimental import pallas as pl
from jax.experimental.pallas import tpu as pltpu
from jax.sharding import PartitionSpec as P

ICE_GROUPS = (4,)
SEA_GROUPS = (3, 3)
EDGE = 16
ICE_CHUNK = 24
SEA_CHUNK = 24
LANES = 128
MESH_ID = pl.DeviceIdType.MESH

U, V, S1, S2, S12, STRENGTH, MASSX, COVER, WX, WY, OU, OV = range(12)
C1, C2, RELAX, INVM, KU, KV = range(6)
LEVEL, TU, TV, DEPTH, LAND, SX, SY = range(7)
ICE_SIGNS = {U: -1.0, V: -1.0}
SEA_SIGNS = {TU: -1.0, TV: -1.0}


class Exchange:
    def __init__(self, name, fields, steps, rows):
        self.name, self.fields, self.steps = name, fields, steps
        self.width = 2 * steps
        lanes = len(fields) * self.width
        self.groups = 4 if lanes <= 32 else 2 if lanes <= 64 else 1
        self.group_lanes = LANES // self.groups
        assert len(fields) * self.width <= self.group_lanes
        self.group_rows = rows // self.groups
        self.extra = name == "ice0"
        count = len(fields) * self.width + (1 if self.extra else 0)
        self.strip_rows = -(-count // 8) * 8

    def scratch(self, blocks):
        f32 = jnp.float32
        packed, got = (self.group_rows, LANES), (self.group_rows + 16, LANES)
        strip = (self.strip_rows, LANES)
        return dict(
            top=pltpu.VMEM(strip, f32),
            bot=pltpu.VMEM(strip, f32),
            low=pltpu.VMEM(strip, f32),
            high=pltpu.VMEM(strip, f32),
            west=pltpu.VMEM(packed, f32),
            east=pltpu.VMEM(packed, f32),
            right=pltpu.VMEM(got, f32),
            left=pltpu.VMEM(got, f32),
            strips=pltpu.VMEM((blocks * self.strip_rows, LANES), f32),
            send=pltpu.SemaphoreType.DMA((8,)),
            recv=pltpu.SemaphoreType.DMA((8,)),
            strip_send=pltpu.SemaphoreType.DMA((blocks,)),
            strip_recv=pltpu.SemaphoreType.DMA((blocks,)),
        )


def plan(rows):
    ice = [Exchange(f"ice{i}", list(range(12 if i == 0 else 5)), s, rows) for i, s in enumerate(ICE_GROUPS)]
    first = Exchange("sea0", [LEVEL, TU, TV, DEPTH, LAND], SEA_GROUPS[0], rows)
    surf = Exchange("surf", [SX, SY], SEA_GROUPS[0], rows)
    later = [Exchange(f"sea{i}", [LEVEL, TU, TV], s, rows) for i, s in enumerate(SEA_GROUPS) if i]
    return ice, first, surf, later


def kernel_body(
    blocks,
    bands,
    names,
    vel_in,
    str_in,
    mass_in,
    strength_in,
    wind_in,
    level_in,
    trans_in,
    depth_in,
    land_in,
    icemask_in,
    partner_in,
    vel_out,
    str_out,
    level_out,
    trans_out,
    *scratch,
):
    ref = dict(zip(names, scratch))
    ice, der, sea, cor = ref["ice"], ref["der"], ref["sea"], ref["cor"]
    ist, ider, sst, sder = ref["ist"], ref["ider"], ref["sst"], ref["sder"]
    masks, partner, perm = ref["masks"], ref["partner"], ref["perm"]
    in_sem, out_sem = ref["in_sem"], ref["out_sem"]
    rows = mass_in.shape[0]
    total_rows = rows * bands
    own = slice(EDGE, EDGE + rows)
    full = rows + 16
    gy, gx = lax.axis_index("gy"), lax.axis_index("gx")
    west_x, east_x = lax.rem(gx + blocks - 1, blocks), lax.rem(gx + 1, blocks)
    is_top, is_low = gy == bands - 1, gy == 0
    ice_ex, sea_ex, surf_ex, later_ex = plan(rows)

    barrier = pltpu.get_barrier_semaphore()

    def greet(y, x):
        pl.semaphore_signal(barrier, inc=1, device_id=(y, x), device_id_type=MESH_ID)

    greet(gy, west_x)
    greet(gy, east_x)

    @pl.when(gy < bands - 1)
    def _():
        for x in (gx, west_x, east_x):
            greet(gy + 1, x)

    @pl.when(gy > 0)
    def _():
        for x in (gx, west_x, east_x):
            greet(gy - 1, x)

    @pl.when(is_top)
    def _():
        def one(j, carry):
            greet(gy, lax.rem(gx + j, blocks))
            return carry

        lax.fori_loop(1, blocks, one, 0)

    loads = [
        (vel_in, ice.at[U : V + 1, 0, own]),
        (str_in, ice.at[S1 : S12 + 1, 0, own]),
        (mass_in, ice.at[MASSX, 0, own]),
        (strength_in, ice.at[STRENGTH, 0, own]),
        (wind_in, ice.at[WX : WY + 1, 0, own]),
        (level_in, sea.at[LEVEL, 0, own]),
        (trans_in, sea.at[TU : TV + 1, 0, own]),
        (depth_in, sea.at[DEPTH, 0, own]),
        (land_in, masks.at[0]),
        (icemask_in, masks.at[1]),
        (partner_in, partner),
    ]
    loads = [pltpu.make_async_copy(a, b, in_sem.at[i]) for i, (a, b) in enumerate(loads)]
    for copy in loads:
        copy.start()

    def loop(count, body):
        for i in range(count):
            body(i)

    def coriolis(i):
        at = i * 8
        r = lax.broadcasted_iota(jnp.int32, (8, LANES), 0) + (gy * rows + at - EDGE)
        angle = jnp.pi * ((r.astype(jnp.float32) + 0.5) / total_rows - 0.5)
        cor[pl.ds(at, 8), :] = 0.5 * jnp.sin(angle)

    loop((rows + 2 * EDGE) // 8, coriolis)
    for copy in loads:
        copy.wait()

    def prepare(i):
        at = i * 8
        here, m = pl.ds(at + EDGE, 8), pl.ds(at, 8)
        land = masks[0, m, :].astype(jnp.float32)
        cover = land * masks[1, m, :].astype(jnp.float32)
        depth = sea[DEPTH, 0, here, :]
        sea[LAND, 0, here, :] = land
        ice[COVER, 0, here, :] = cover
        ice[MASSX, 0, here, :] = ice[MASSX, 0, here, :] + 1.0 - cover
        ice[OU, 0, here, :] = sea[TU, 0, here, :] / depth
        ice[OV, 0, here, :] = sea[TV, 0, here, :] / depth

    loop(rows // 8, prepare)

    lane8 = lax.broadcasted_iota(jnp.int32, (8, LANES), 1)

    def stage(ex, store):
        w = ex.width
        top, bot = ref[ex.name, "top"], ref[ex.name, "bot"]
        for k, f in enumerate(ex.fields):
            top[k * w : (k + 1) * w, :] = store[f, 0, EDGE + rows - w : EDGE + rows, :]
            bot[k * w : (k + 1) * w, :] = store[f, 0, EDGE : EDGE + w, :]
        if ex.extra:
            at = len(ex.fields) * w
            local = partner[...] - (blocks - 1 - gx) * LANES
            top[at : at + 1, :] = local.astype(jnp.float32)

        def pack(i):
            to_west = to_east = None
            for g in range(ex.groups):
                for k, f in enumerate(ex.fields):
                    at = g * ex.group_lanes + k * w
                    here = pl.ds(EDGE + g * ex.group_rows + i * 8, 8)
                    x = store[f, 0, here, :]
                    a = pltpu.roll(x, at, 1) if at else x
                    b = pltpu.roll(x, (at + w) % LANES, 1) if (at + w) % LANES else x
                    if to_west is None:
                        to_west, to_east = a, b
                    else:
                        keep = lane8 < at
                        to_west = jnp.where(keep, to_west, a)
                        to_east = jnp.where(keep, to_east, b)
            m = pl.ds(i * 8, 8)
            ref[ex.name, "west"][m, :] = to_west
            ref[ex.name, "east"][m, :] = to_east

        loop(ex.group_rows // 8, pack)

    def sends(ex):
        r = lambda part: ref[ex.name, part]
        n = ex.group_rows
        last, first = pl.ds(n - 8, 8), pl.ds(0, 8)
        mid, low, high = pl.ds(0, n), pl.ds(n, 8), pl.ds(n + 8, 8)
        up, down, flat = 1, -1, 0
        table = [
            (r("top"), r("low"), up, gx),
            (r("bot"), r("high"), down, gx),
            (r("west"), r("right").at[mid], flat, west_x),
            (r("east"), r("left").at[mid], flat, east_x),
            (r("west").at[last], r("right").at[low], up, west_x),
            (r("east").at[last], r("left").at[low], up, east_x),
            (r("west").at[first], r("right").at[high], down, west_x),
            (r("east").at[first], r("left").at[high], down, east_x),
        ]
        out = []
        for i, (src, dst, dy, x) in enumerate(table):
            copy = pltpu.make_async_remote_copy(
                src_ref=src,
                dst_ref=dst,
                send_sem=r("send").at[i],
                recv_sem=r("recv").at[i],
                device_id=(gy + dy, x),
                device_id_type=MESH_ID,
            )
            out.append((dy, copy))
        return out

    def strip_copy(ex, target, source):
        n = ex.strip_rows
        return pltpu.make_async_remote_copy(
            src_ref=ref[ex.name, "top"],
            dst_ref=ref[ex.name, "strips"].at[pl.ds(pl.multiple_of(source * n, 8), n)],
            send_sem=ref[ex.name, "strip_send"].at[target],
            recv_sem=ref[ex.name, "strip_recv"].at[source],
            device_id=(gy, target),
            device_id_type=MESH_ID,
        )

    def each_strip(ex, action):
        reach = ex.steps

        @pl.when(is_top)
        def _():
            def one(j, carry):
                x = lax.rem(gx + j, blocks)
                gap = lax.rem(x + gx + 1, blocks)
                near = (j <= reach) | (j >= blocks - reach) | (gap <= reach) | (gap >= blocks - reach)

                @pl.when(near)
                def _():
                    action(x)

                return carry

            lax.fori_loop(1, blocks, one, 0)

    def start(ex):
        each_strip(ex, lambda x: strip_copy(ex, x, gx).start())
        copies = sends(ex)
        for dy in (0, 1, -1):
            chosen = [c for d, c in copies if d == dy]

            def go(chosen=chosen):
                for c in chosen:
                    c.start()

            if dy == 0:
                go()
            else:
                pl.when((gy < bands - 1) if dy > 0 else (gy > 0))(go)
        n = ex.strip_rows

        @pl.when(is_top)
        def _():
            ref[ex.name, "strips"][pl.ds(pl.multiple_of(gx * n, 8), n), :] = ref[ex.name, "top"][...]

    def wait_recv(ex):
        copies = sends(ex)
        for dy in (0, 1, -1):
            chosen = [c for d, c in copies if d == dy]

            def go(chosen=chosen):
                for c in chosen:
                    c.wait_recv()

            if dy == 0:
                go()
            else:
                pl.when((gy > 0) if dy > 0 else (gy < bands - 1))(go)

    def wait_strips(ex):
        each_strip(ex, lambda x: strip_copy(ex, gx, x).wait_recv())

    def wait_send(ex):
        copies = sends(ex)
        for dy in (0, 1, -1):
            chosen = [c for d, c in copies if d == dy]

            def go(chosen=chosen):
                for c in chosen:
                    c.wait_send()

            if dy == 0:
                go()
            else:
                pl.when((gy < bands - 1) if dy > 0 else (gy > 0))(go)
        each_strip(ex, lambda x: strip_copy(ex, x, gx).wait_send())

    def unpack(ex, store, ones):
        w, n = ex.width, ex.group_rows
        right, left = ref[ex.name, "right"], ref[ex.name, "left"]

        def place(source, g, target):
            x, y = right[source, :], left[source, :]
            for k, f in enumerate(ex.fields):
                at = g * ex.group_lanes + k * w
                a = pltpu.roll(x, (LANES - at) % LANES, 1) if at else x
                shift = (2 * LANES - w - at) % LANES
                b = pltpu.roll(y, shift, 1) if shift else y
                store[f, 1, target, :] = jnp.where(lane8 < LANES // 2, a, b)

        def main(i):
            source = pl.ds(i * 8, 8)
            for g in range(ex.groups):
                place(source, g, pl.ds(EDGE + g * n + i * 8, 8))

        loop(n // 8, main)

        @pl.when(gy > 0)
        def _():
            place(pl.ds(n, 8), ex.groups - 1, pl.ds(EDGE - 8, 8))
            for k, f in enumerate(ex.fields):
                store[f, 0, EDGE - w : EDGE, :] = ref[ex.name, "low"][k * w : (k + 1) * w, :]

        @pl.when(gy < bands - 1)
        def _():
            place(pl.ds(n + 8, 8), 0, pl.ds(EDGE + rows, 8))
            for k, f in enumerate(ex.fields):
                store[f, 0, EDGE + rows : EDGE + rows + w, :] = ref[ex.name, "high"][k * w : (k + 1) * w, :]

        @pl.when(is_low)
        def _():
            for f in ex.fields:
                fill = jnp.full((8, LANES), 1.0 if f == ones else 0.0, jnp.float32)
                store[f, 0, EDGE - 8 : EDGE, :] = fill
                store[f, 1, EDGE - 8 : EDGE, :] = fill

    blane = lax.broadcasted_iota(jnp.int32, (blocks, LANES), 1)
    turn = 7 - lax.broadcasted_iota(jnp.int32, (8, LANES), 0)

    def strip_load(ex, strip):
        w, n = ex.width, ex.strip_rows
        got = ref[ex.name, "strips"]
        for k, f in enumerate(ex.fields):
            for d in range(w):
                strip[f, 2 + d] = got[pl.ds(k * w + w - 1 - d, blocks, stride=n), :]
        if ex.extra:
            perm[...] = got[pl.ds(len(ex.fields) * w, blocks, stride=n), :].astype(jnp.int32)

    def fold_rows(x):
        parts = [jnp.take_along_axis(x[b : b + 8], turn, axis=0) for b in range(blocks - 8, -1, -8)]
        index = perm[...]
        parts = [jnp.take_along_axis(p, index[8 * i : 8 * i + 8], axis=1) for i, p in enumerate(parts)]
        return jnp.concatenate(parts, axis=0)

    def fold(strip, store, fields, signs):
        for f in fields:
            for k in (0, 1):
                x = fold_rows(strip[f, 2 + k])
                strip[f, 1 - k] = -x if f in signs else x
        lane1 = lax.broadcasted_iota(jnp.int32, (1, LANES), 1)
        for f in fields:
            for k in (0, 1):
                row = slice(EDGE + rows + k, EDGE + rows + k + 1)
                store[f, 0, row, :] = strip[f, 1 - k, pl.ds(gx, 1), :]
                store[f, 1, row, :] = jnp.where(
                    lane1 < LANES // 2, strip[f, 1 - k, pl.ds(east_x, 1), :], strip[f, 1 - k, pl.ds(west_x, 1), :]
                )

    def dx_strip(x):
        a = jnp.where(blane == 0, pltpu.roll(x, blocks - 1, 0), x)
        b = jnp.where(blane == LANES - 1, pltpu.roll(x, 1, 0), x)
        return pltpu.roll(a, LANES - 1, 1) - pltpu.roll(b, 1, 1)

    def row_coriolis(i):
        row = total_rows + 1 - i
        return 0.5 * math.sin(math.pi * ((row + 0.5) / total_rows - 0.5))

    def ice_coefficients(strength, massx, cover, u, v, wx, wy):
        relax = 2.0 + jnp.sqrt(16.0 * strength / massx)
        share = cover / (1.0 + relax)
        inv = 1.0 / massx
        return share * relax, share * strength, relax, inv, u + wx * inv, v + wy * inv

    def stresses(exx, eyy, shear, c1, c2, s1, s2, s12):
        div, ten = exx + eyy, exx - eyy
        r = lax.rsqrt(div * div + (ten * ten + shear * shear) * 0.25 + 0.01)
        g = c2 * r
        return c1 * s1 + (g * div - c2), c1 * s2 + (0.25 * g) * ten, c1 * s12 + (0.125 * g) * shear

    def velocities(fx, fy, u, v, relax, inv, cover, ku, kv, ou, ov, f):
        rx, ry = ou - u, ov - v
        drag = 0.5 * jnp.sqrt(rx * rx + ry * ry)
        part = cover / (1.0 + relax + drag * inv)
        new_u = part * (relax * u + ku + inv * (fx + drag * ou) + f * v)
        new_v = part * (relax * v + kv + inv * (fy + drag * ov) - f * u)
        return new_u, new_v

    def dx_pair(m, h, first, last):
        am, ah = jnp.where(first, h, m), jnp.where(first, m, h)
        bm, bh = jnp.where(last, h, m), jnp.where(last, m, h)
        return (
            pltpu.roll(am, LANES - 1, 1) - pltpu.roll(bm, 1, 1),
            pltpu.roll(ah, LANES - 1, 1) - pltpu.roll(bh, 1, 1),
        )

    def ends(chunk):
        lane = lax.broadcasted_iota(jnp.int32, (chunk, LANES), 1)
        return lane == 0, lane == LANES - 1

    def ice_static(i):
        here = pl.ds(EDGE - 8 + i * 8, 8)
        for p in (0, 1):
            got = ice_coefficients(*(ice[f, p, here, :] for f in (STRENGTH, MASSX, COVER, U, V, WX, WY)))
            for f, x in enumerate(got):
                der[f, p, here, :] = x

    def dx_own(m, h, first, last):
        am, bm = jnp.where(first, h, m), jnp.where(last, h, m)
        return (pltpu.roll(am, LANES - 1, 1) - pltpu.roll(bm, 1, 1),)

    def ice_step(final):
        n = ICE_CHUNK
        planes, dx = ((0,), dx_own) if final else ((0, 1), dx_pair)
        first, last = ends(n)

        def stress(i):
            at = EDGE - 8 + i * n
            here, north, south = pl.ds(at, n), pl.ds(at + 1, n), pl.ds(at - 1, n)
            exx = dx_pair(ice[U, 0, here, :], ice[U, 1, here, :], first, last)
            exv = dx_pair(ice[V, 0, here, :], ice[V, 1, here, :], first, last)
            for p in (0, 1):
                eyy = ice[V, p, north, :] - ice[V, p, south, :]
                shear = ice[U, p, north, :] - ice[U, p, south, :] + exv[p]
                got = stresses(
                    exx[p], eyy, shear, der[C1, p, here, :], der[C2, p, here, :], *(ice[f, p, here, :] for f in (S1, S2, S12))
                )
                for f, x in zip((S1, S2, S12), got):
                    ice[f, p, here, :] = x

        loop(full // n, stress)

        def velocity(i):
            at = EDGE - 8 + i * n
            here, north, south = pl.ds(at, n), pl.ds(at + 1, n), pl.ds(at - 1, n)
            sums = [ice[S1, p, here, :] + ice[S2, p, here, :] for p in (0, 1)]
            dsum = dx(sums[0], sums[1], first, last)
            dxy = dx(ice[S12, 0, here, :], ice[S12, 1, here, :], first, last)
            f = cor[here, :]
            for p in planes:
                fx = 0.25 * dsum[p] + 0.5 * (ice[S12, p, north, :] - ice[S12, p, south, :])
                dyy = (ice[S1, p, north, :] - ice[S2, p, north, :]) - (ice[S1, p, south, :] - ice[S2, p, south, :])
                fy = 0.5 * dxy[p] + 0.25 * dyy
                u, v = ice[U, p, here, :], ice[V, p, here, :]
                new_u, new_v = velocities(
                    fx,
                    fy,
                    u,
                    v,
                    der[RELAX, p, here, :],
                    der[INVM, p, here, :],
                    ice[COVER, p, here, :],
                    der[KU, p, here, :],
                    der[KV, p, here, :],
                    ice[OU, p, here, :],
                    ice[OV, p, here, :],
                    f,
                )
                ice[U, p, here, :] = new_u
                ice[V, p, here, :] = new_v

        loop(full // n, velocity)

    def ice_strip_static(w):
        for i in range(1, w + 2):
            fields = (STRENGTH, MASSX, COVER, U, V, WX, WY)
            got = ice_coefficients(*(ist[f, i] for f in fields))
            for f, x in enumerate(got):
                ider[f, i] = x

    def ice_strip_step(n):
        for i in range(1, n + 1):
            exx, exv = dx_strip(ist[U, i]), dx_strip(ist[V, i])
            eyy = ist[V, i - 1] - ist[V, i + 1]
            shear = ist[U, i - 1] - ist[U, i + 1] + exv
            got = stresses(exx, eyy, shear, ider[C1, i], ider[C2, i], *(ist[f, i] for f in (S1, S2, S12)))
            for f, x in zip((S1, S2, S12), got):
                ist[f, i] = x
        for i in range(2, n):
            fx = 0.25 * dx_strip(ist[S1, i] + ist[S2, i]) + 0.5 * (ist[S12, i - 1] - ist[S12, i + 1])
            dyy = (ist[S1, i - 1] - ist[S2, i - 1]) - (ist[S1, i + 1] - ist[S2, i + 1])
            fy = 0.5 * dx_strip(ist[S12, i]) + 0.25 * dyy
            new_u, new_v = velocities(
                fx,
                fy,
                ist[U, i],
                ist[V, i],
                ider[RELAX, i],
                ider[INVM, i],
                ist[COVER, i],
                ider[KU, i],
                ider[KV, i],
                ist[OU, i],
                ist[OV, i],
                row_coriolis(i),
            )
            ist[U, i] = new_u
            ist[V, i] = new_v

    def sea_coefficients(depth, land):
        return land / (1.0 + 0.1 / depth), 0.25 * depth

    def sea_static(i):
        here = pl.ds(EDGE - 8 + i * 8, 8)
        for p in (0, 1):
            a, b = sea_coefficients(sea[DEPTH, p, here, :], sea[LAND, p, here, :])
            der[0, p, here, :] = a
            der[1, p, here, :] = b

    def flows(tu, tv, part, slope, dlx, dly, f, sx, sy):
        east = part * (tu - slope * dlx + (0.5 * f) * tv + 0.5 * sx)
        north = part * (tv - slope * dly - (0.5 * f) * tu + 0.5 * sy)
        return east, north

    def sea_step(final):
        n = SEA_CHUNK
        planes, dx = ((0,), dx_own) if final else ((0, 1), dx_pair)
        first, last = ends(n)

        def level(i):
            at = EDGE - 8 + i * n
            here, north, south = pl.ds(at, n), pl.ds(at + 1, n), pl.ds(at - 1, n)
            du = dx_pair(sea[TU, 0, here, :], sea[TU, 1, here, :], first, last)
            for p in (0, 1):
                dv = sea[TV, p, north, :] - sea[TV, p, south, :]
                sea[LEVEL, p, here, :] = sea[LAND, p, here, :] * (sea[LEVEL, p, here, :] - 0.25 * (du[p] + dv))

        loop(full // n, level)

        def flow(i):
            at = EDGE - 8 + i * n
            here, north, south = pl.ds(at, n), pl.ds(at + 1, n), pl.ds(at - 1, n)
            dlx = dx(sea[LEVEL, 0, here, :], sea[LEVEL, 1, here, :], first, last)
            f = cor[here, :]
            for p in planes:
                dly = sea[LEVEL, p, north, :] - sea[LEVEL, p, south, :]
                east, nrth = flows(
                    sea[TU, p, here, :],
                    sea[TV, p, here, :],
                    der[0, p, here, :],
                    der[1, p, here, :],
                    dlx[p],
                    dly,
                    f,
                    sea[SX, p, here, :],
                    sea[SY, p, here, :],
                )
                sea[TU, p, here, :] = east
                sea[TV, p, here, :] = nrth

        loop(full // n, flow)

    def sea_strip_static(w):
        for i in range(2, w + 2):
            a, b = sea_coefficients(sst[DEPTH, i], sst[LAND, i])
            sder[0, i] = a
            sder[1, i] = b

    def sea_strip_step(n):
        for i in range(1, n + 1):
            dv = sst[TV, i - 1] - sst[TV, i + 1]
            sst[LEVEL, i] = sst[LAND, i] * (sst[LEVEL, i] - 0.25 * (dx_strip(sst[TU, i]) + dv))
        for i in range(2, n):
            dly = sst[LEVEL, i - 1] - sst[LEVEL, i + 1]
            east, nrth = flows(
                sst[TU, i],
                sst[TV, i],
                sder[0, i],
                sder[1, i],
                dx_strip(sst[LEVEL, i]),
                dly,
                row_coriolis(i),
                sst[SX, i],
                sst[SY, i],
            )
            sst[TU, i] = east
            sst[TV, i] = nrth

    stage(ice_ex[0], ice)
    greeted = 2 + 3 * (gy < bands - 1).astype(jnp.int32) + 3 * (gy > 0).astype(jnp.int32)
    pl.semaphore_wait(barrier, greeted + (blocks - 1) * is_top.astype(jnp.int32))
    start(ice_ex[0])
    stage(sea_ex, sea)
    start(sea_ex)

    state = (U, V, S1, S2, S12)
    for number, ex in enumerate(ice_ex):
        if number:
            stage(ex, ice)
            start(ex)
        wait_recv(ex)
        unpack(ex, ice, MASSX)
        wait_strips(ex)

        @pl.when(is_top)
        def _(ex=ex, number=number):
            strip_load(ex, ist)
            fold(ist, ice, state + ((STRENGTH, MASSX, COVER, WX, WY) if number == 0 else ()), ICE_SIGNS)
            if number == 0:
                ice_strip_static(ex.width)

        if number == 0:
            loop(full // 8, ice_static)
        for step in range(ex.steps):
            if step:

                @pl.when(is_top)
                def _(n=ex.width - 2 * (step - 1)):
                    ice_strip_step(n)
                    fold(ist, ice, state, ICE_SIGNS)

            ice_step(step == ex.steps - 1)

    def surface(i):
        here = pl.ds(EDGE + i * 8, 8)
        cover = ice[COVER, 0, here, :]
        rx, ry = ice[U, 0, here, :] - ice[OU, 0, here, :], ice[V, 0, here, :] - ice[OV, 0, here, :]
        drag = cover * (0.5 * jnp.sqrt(rx * rx + ry * ry))
        sea[SX, 0, here, :] = drag * rx + (1.0 - cover) * ice[WX, 0, here, :]
        sea[SY, 0, here, :] = drag * ry + (1.0 - cover) * ice[WY, 0, here, :]

    loop(rows // 8, surface)
    stage(surf_ex, sea)
    start(surf_ex)
    outs = [
        pltpu.make_async_copy(ice.at[U : V + 1, 0, own], vel_out, out_sem.at[0]),
        pltpu.make_async_copy(ice.at[S1 : S12 + 1, 0, own], str_out, out_sem.at[1]),
        pltpu.make_async_copy(sea.at[LEVEL, 0, own], level_out, out_sem.at[2]),
        pltpu.make_async_copy(sea.at[TU : TV + 1, 0, own], trans_out, out_sem.at[3]),
    ]
    for copy in outs[:2]:
        copy.start()
    flow_state = (LEVEL, TU, TV)
    for number, ex in enumerate([sea_ex] + later_ex):
        if number:
            stage(ex, sea)
            start(ex)
        wait_recv(ex)
        unpack(ex, sea, DEPTH)
        wait_strips(ex)

        @pl.when(is_top)
        def _(ex=ex, number=number):
            strip_load(ex, sst)
            fold(sst, sea, flow_state + ((DEPTH, LAND) if number == 0 else ()), SEA_SIGNS)
            if number == 0:
                sea_strip_static(ex.width)

        if number == 0:
            loop(full // 8, sea_static)
            wait_recv(surf_ex)
            unpack(surf_ex, sea, DEPTH)
            wait_strips(surf_ex)

            @pl.when(is_top)
            def _():
                strip_load(surf_ex, sst)

        for step in range(ex.steps):
            if step:

                @pl.when(is_top)
                def _(n=ex.width - 2 * (step - 1)):
                    sea_strip_step(n)
                    fold(sst, sea, flow_state, SEA_SIGNS)

            sea_step(step == ex.steps - 1)

    for copy in outs[2:]:
        copy.start()
    for ex in ice_ex + [sea_ex, surf_ex] + later_ex:
        wait_send(ex)
    for copy in outs:
        copy.wait()


def write_out(*refs):
    sources, targets, held, sems = refs[:4], refs[4:8], refs[8:12], refs[12]
    pairs = list(zip(sources, held, targets))
    reads = [pltpu.make_async_copy(a, b, sems.at[0, i]) for i, (a, b, _) in enumerate(pairs)]
    writes = [pltpu.make_async_copy(b, c, sems.at[1, i]) for i, (_, b, c) in enumerate(pairs)]
    for copy in reads:
        copy.start()
    for read, write in zip(reads, writes):
        read.wait()
        write.start()
    for copy in writes:
        copy.wait()


def per_device(blocks, bands, *args):
    f32 = jnp.float32
    rows = args[2].shape[0]
    tall = rows + 2 * EDGE
    ice_ex, sea_ex, surf_ex, later_ex = plan(rows)
    depth = 2 + 2 * max(ICE_GROUPS + SEA_GROUPS)
    scratch = dict(
        ice=pltpu.VMEM((12, 2, tall, LANES), f32),
        der=pltpu.VMEM((6, 2, tall, LANES), f32),
        sea=pltpu.VMEM((7, 2, tall, LANES), f32),
        cor=pltpu.VMEM((tall, LANES), f32),
        ist=pltpu.VMEM((12, depth, blocks, LANES), f32),
        ider=pltpu.VMEM((6, depth, blocks, LANES), f32),
        sst=pltpu.VMEM((7, depth, blocks, LANES), f32),
        sder=pltpu.VMEM((2, depth, blocks, LANES), f32),
        masks=pltpu.VMEM((2, rows, LANES), jnp.int32),
        partner=pltpu.VMEM((1, LANES), jnp.int32),
        perm=pltpu.VMEM((blocks, LANES), jnp.int32),
        in_sem=pltpu.SemaphoreType.DMA((11,)),
        out_sem=pltpu.SemaphoreType.DMA((4,)),
    )
    for ex in ice_ex + [sea_ex, surf_ex] + later_ex:
        for part, space in ex.scratch(blocks).items():
            scratch[ex.name, part] = space

    def body(*refs):
        kernel_body(blocks, bands, list(scratch), *refs)

    sds = jax.ShapeDtypeStruct
    args = args[:-1] + (args[-1].reshape(1, LANES),)
    shapes = (
        sds((2, rows, LANES), f32),
        sds((3, rows, LANES), f32),
        sds((rows, LANES), f32),
        sds((2, rows, LANES), f32),
    )
    far = pl.BlockSpec(memory_space=pltpu.HBM)
    results = pl.pallas_call(
        body,
        out_shape=shapes,
        in_specs=[far] * 11,
        out_specs=(far,) * 4,
        scratch_shapes=list(scratch.values()),
        compiler_params=pltpu.CompilerParams(
            collective_id=0, has_side_effects=True, vmem_limit_bytes=67043328
        ),
        name="coupled_step",
    )(*args)
    return pl.pallas_call(
        write_out,
        out_shape=shapes,
        in_specs=[far] * 4,
        out_specs=(far,) * 4,
        scratch_shapes=[pltpu.VMEM(x.shape, f32) for x in shapes] + [pltpu.SemaphoreType.DMA((2, 4))],
        compiler_params=pltpu.CompilerParams(vmem_limit_bytes=67043328),
        name="write_out",
    )(*results)


def solution(mesh):
    blocks, bands = mesh.shape["gx"], mesh.shape["gy"]
    flat, stacked = P("gy", "gx"), P(None, "gy", "gx")
    in_specs = (stacked, stacked, flat, flat, stacked, flat, stacked, flat, flat, flat, P("gx"))

    def step(*args):
        return per_device(blocks, bands, *args)

    return jax.shard_map(
        step, mesh=mesh, in_specs=in_specs, out_specs=(stacked, stacked, flat, stacked), check_vma=False
    )
```

```python
import math

import jax
import jax.numpy as jnp
from jax import lax
from jax.experimental import pallas as pl
from jax.experimental.pallas import tpu as pltpu
from jax.sharding import PartitionSpec as P

ICE_GROUPS = (4,)
SEA_GROUPS = (3, 3)
EDGE = 16
ICE_CHUNK = 24
SEA_CHUNK = 24
LANES = 128
MESH_ID = pl.DeviceIdType.MESH

U, V, S1, S2, S12, STRENGTH, MASSX, COVER, WX, WY, OU, OV = range(12)
C1, C2, RELAX, INVM, KU, KV = range(6)
LEVEL, TU, TV, DEPTH, LAND, SX, SY = range(7)
ICE_SIGNS = {U: -1.0, V: -1.0}
SEA_SIGNS = {TU: -1.0, TV: -1.0}


class Exchange:
    def __init__(self, name, fields, steps, rows):
        self.name, self.fields, self.steps = name, fields, steps
        self.width = 2 * steps
        lanes = len(fields) * self.width
        self.groups = 4 if lanes <= 32 else 2 if lanes <= 64 else 1
        self.group_lanes = LANES // self.groups
        assert len(fields) * self.width <= self.group_lanes
        self.group_rows = rows // self.groups
        self.extra = name == "ice0"
        count = len(fields) * self.width + (1 if self.extra else 0)
        self.strip_rows = -(-count // 8) * 8

    def scratch(self, blocks):
        f32 = jnp.float32
        packed, got = (self.group_rows, LANES), (self.group_rows + 16, LANES)
        strip = (self.strip_rows, LANES)
        return dict(
            top=pltpu.VMEM(strip, f32),
            bot=pltpu.VMEM(strip, f32),
            low=pltpu.VMEM(strip, f32),
            high=pltpu.VMEM(strip, f32),
            west=pltpu.VMEM(packed, f32),
            east=pltpu.VMEM(packed, f32),
            right=pltpu.VMEM(got, f32),
            left=pltpu.VMEM(got, f32),
            strips=pltpu.VMEM((blocks * self.strip_rows, LANES), f32),
            send=pltpu.SemaphoreType.DMA((8,)),
            recv=pltpu.SemaphoreType.DMA((8,)),
            strip_send=pltpu.SemaphoreType.DMA((blocks,)),
            strip_recv=pltpu.SemaphoreType.DMA((blocks,)),
        )


def plan(rows):
    ice = [Exchange(f"ice{i}", list(range(12 if i == 0 else 5)), s, rows) for i, s in enumerate(ICE_GROUPS)]
    first = Exchange("sea0", [LEVEL, TU, TV, DEPTH, LAND], SEA_GROUPS[0], rows)
    surf = Exchange("surf", [SX, SY], SEA_GROUPS[0], rows)
    later = [Exchange(f"sea{i}", [LEVEL, TU, TV], s, rows) for i, s in enumerate(SEA_GROUPS) if i]
    return ice, first, surf, later


def kernel_body(
    blocks,
    bands,
    names,
    vel_in,
    str_in,
    mass_in,
    strength_in,
    wind_in,
    level_in,
    trans_in,
    depth_in,
    land_in,
    icemask_in,
    partner_in,
    vel_out,
    str_out,
    level_out,
    trans_out,
    *scratch,
):
    ref = dict(zip(names, scratch))
    ice, der, sea, cor = ref["ice"], ref["der"], ref["sea"], ref["cor"]
    ist, ider, sst, sder = ref["ist"], ref["ider"], ref["sst"], ref["sder"]
    masks, partner, perm = ref["masks"], ref["partner"], ref["perm"]
    in_sem, out_sem = ref["in_sem"], ref["out_sem"]
    rows = mass_in.shape[0]
    total_rows = rows * bands
    own = slice(EDGE, EDGE + rows)
    full = rows + 16
    gy, gx = lax.axis_index("gy"), lax.axis_index("gx")
    west_x, east_x = lax.rem(gx + blocks - 1, blocks), lax.rem(gx + 1, blocks)
    is_top, is_low = gy == bands - 1, gy == 0
    ice_ex, sea_ex, surf_ex, later_ex = plan(rows)

    barrier = pltpu.get_barrier_semaphore()

    def greet(y, x):
        pl.semaphore_signal(barrier, inc=1, device_id=(y, x), device_id_type=MESH_ID)

    greet(gy, west_x)
    greet(gy, east_x)

    @pl.when(gy < bands - 1)
    def _():
        for x in (gx, west_x, east_x):
            greet(gy + 1, x)

    @pl.when(gy > 0)
    def _():
        for x in (gx, west_x, east_x):
            greet(gy - 1, x)

    @pl.when(is_top)
    def _():
        def one(j, carry):
            greet(gy, lax.rem(gx + j, blocks))
            return carry

        lax.fori_loop(1, blocks, one, 0)

    loads = [
        (vel_in, ice.at[U : V + 1, 0, own]),
        (str_in, ice.at[S1 : S12 + 1, 0, own]),
        (mass_in, ice.at[MASSX, 0, own]),
        (strength_in, ice.at[STRENGTH, 0, own]),
        (wind_in, ice.at[WX : WY + 1, 0, own]),
        (level_in, sea.at[LEVEL, 0, own]),
        (trans_in, sea.at[TU : TV + 1, 0, own]),
        (depth_in, sea.at[DEPTH, 0, own]),
        (land_in, masks.at[0]),
        (icemask_in, masks.at[1]),
        (partner_in, partner),
    ]
    loads = [pltpu.make_async_copy(a, b, in_sem.at[i]) for i, (a, b) in enumerate(loads)]
    for copy in loads:
        copy.start()

    def loop(count, body):
        for i in range(count):
            body(i)

    def coriolis(i):
        at = i * 8
        r = lax.broadcasted_iota(jnp.int32, (8, LANES), 0) + (gy * rows + at - EDGE)
        angle = jnp.pi * ((r.astype(jnp.float32) + 0.5) / total_rows - 0.5)
        cor[pl.ds(at, 8), :] = 0.5 * jnp.sin(angle)

    loop((rows + 2 * EDGE) // 8, coriolis)
    for copy in loads:
        copy.wait()

    def prepare(i):
        at = i * 8
        here, m = pl.ds(at + EDGE, 8), pl.ds(at, 8)
        land = masks[0, m, :].astype(jnp.float32)
        cover = land * masks[1, m, :].astype(jnp.float32)
        depth = sea[DEPTH, 0, here, :]
        sea[LAND, 0, here, :] = land
        ice[COVER, 0, here, :] = cover
        ice[MASSX, 0, here, :] = ice[MASSX, 0, here, :] + 1.0 - cover
        ice[OU, 0, here, :] = sea[TU, 0, here, :] / depth
        ice[OV, 0, here, :] = sea[TV, 0, here, :] / depth

    loop(rows // 8, prepare)

    lane8 = lax.broadcasted_iota(jnp.int32, (8, LANES), 1)

    def stage(ex, store):
        w = ex.width
        top, bot = ref[ex.name, "top"], ref[ex.name, "bot"]
        for k, f in enumerate(ex.fields):
            top[k * w : (k + 1) * w, :] = store[f, 0, EDGE + rows - w : EDGE + rows, :]
            bot[k * w : (k + 1) * w, :] = store[f, 0, EDGE : EDGE + w, :]
        if ex.extra:
            at = len(ex.fields) * w
            local = partner[...] - (blocks - 1 - gx) * LANES
            top[at : at + 1, :] = local.astype(jnp.float32)

        def pack(i):
            to_west = to_east = None
            for g in range(ex.groups):
                for k, f in enumerate(ex.fields):
                    at = g * ex.group_lanes + k * w
                    here = pl.ds(EDGE + g * ex.group_rows + i * 8, 8)
                    x = store[f, 0, here, :]
                    a = pltpu.roll(x, at, 1) if at else x
                    b = pltpu.roll(x, (at + w) % LANES, 1) if (at + w) % LANES else x
                    if to_west is None:
                        to_west, to_east = a, b
                    else:
                        keep = lane8 < at
                        to_west = jnp.where(keep, to_west, a)
                        to_east = jnp.where(keep, to_east, b)
            m = pl.ds(i * 8, 8)
            ref[ex.name, "west"][m, :] = to_west
            ref[ex.name, "east"][m, :] = to_east

        loop(ex.group_rows // 8, pack)

    def sends(ex):
        r = lambda part: ref[ex.name, part]
        n = ex.group_rows
        last, first = pl.ds(n - 8, 8), pl.ds(0, 8)
        mid, low, high = pl.ds(0, n), pl.ds(n, 8), pl.ds(n + 8, 8)
        up, down, flat = 1, -1, 0
        table = [
            (r("top"), r("low"), up, gx),
            (r("bot"), r("high"), down, gx),
            (r("west"), r("right").at[mid], flat, west_x),
            (r("east"), r("left").at[mid], flat, east_x),
            (r("west").at[last], r("right").at[low], up, west_x),
            (r("east").at[last], r("left").at[low], up, east_x),
            (r("west").at[first], r("right").at[high], down, west_x),
            (r("east").at[first], r("left").at[high], down, east_x),
        ]
        out = []
        for i, (src, dst, dy, x) in enumerate(table):
            copy = pltpu.make_async_remote_copy(
                src_ref=src,
                dst_ref=dst,
                send_sem=r("send").at[i],
                recv_sem=r("recv").at[i],
                device_id=(gy + dy, x),
                device_id_type=MESH_ID,
            )
            out.append((dy, copy))
        return out

    def strip_copy(ex, target, source):
        n = ex.strip_rows
        return pltpu.make_async_remote_copy(
            src_ref=ref[ex.name, "top"],
            dst_ref=ref[ex.name, "strips"].at[pl.ds(pl.multiple_of(source * n, 8), n)],
            send_sem=ref[ex.name, "strip_send"].at[target],
            recv_sem=ref[ex.name, "strip_recv"].at[source],
            device_id=(gy, target),
            device_id_type=MESH_ID,
        )

    def each_strip(ex, action):
        reach = ex.steps

        @pl.when(is_top)
        def _():
            def one(j, carry):
                x = lax.rem(gx + j, blocks)
                gap = lax.rem(x + gx + 1, blocks)
                near = (j <= reach) | (j >= blocks - reach) | (gap <= reach) | (gap >= blocks - reach)

                @pl.when(near)
                def _():
                    action(x)

                return carry

            lax.fori_loop(1, blocks, one, 0)

    def start(ex):
        each_strip(ex, lambda x: strip_copy(ex, x, gx).start())
        copies = sends(ex)
        for dy in (0, 1, -1):
            chosen = [c for d, c in copies if d == dy]

            def go(chosen=chosen):
                for c in chosen:
                    c.start()

            if dy == 0:
                go()
            else:
                pl.when((gy < bands - 1) if dy > 0 else (gy > 0))(go)
        n = ex.strip_rows

        @pl.when(is_top)
        def _():
            ref[ex.name, "strips"][pl.ds(pl.multiple_of(gx * n, 8), n), :] = ref[ex.name, "top"][...]

    def wait_recv(ex):
        copies = sends(ex)
        for dy in (0, 1, -1):
            chosen = [c for d, c in copies if d == dy]

            def go(chosen=chosen):
                for c in chosen:
                    c.wait_recv()

            if dy == 0:
                go()
            else:
                pl.when((gy > 0) if dy > 0 else (gy < bands - 1))(go)

    def wait_strips(ex):
        each_strip(ex, lambda x: strip_copy(ex, gx, x).wait_recv())

    def wait_send(ex):
        copies = sends(ex)
        for dy in (0, 1, -1):
            chosen = [c for d, c in copies if d == dy]

            def go(chosen=chosen):
                for c in chosen:
                    c.wait_send()

            if dy == 0:
                go()
            else:
                pl.when((gy < bands - 1) if dy > 0 else (gy > 0))(go)
        each_strip(ex, lambda x: strip_copy(ex, x, gx).wait_send())

    def unpack(ex, store, ones):
        w, n = ex.width, ex.group_rows
        right, left = ref[ex.name, "right"], ref[ex.name, "left"]

        def place(source, g, target):
            x, y = right[source, :], left[source, :]
            for k, f in enumerate(ex.fields):
                at = g * ex.group_lanes + k * w
                a = pltpu.roll(x, (LANES - at) % LANES, 1) if at else x
                shift = (2 * LANES - w - at) % LANES
                b = pltpu.roll(y, shift, 1) if shift else y
                store[f, 1, target, :] = jnp.where(lane8 < LANES // 2, a, b)

        def main(i):
            source = pl.ds(i * 8, 8)
            for g in range(ex.groups):
                place(source, g, pl.ds(EDGE + g * n + i * 8, 8))

        loop(n // 8, main)

        @pl.when(gy > 0)
        def _():
            place(pl.ds(n, 8), ex.groups - 1, pl.ds(EDGE - 8, 8))
            for k, f in enumerate(ex.fields):
                store[f, 0, EDGE - w : EDGE, :] = ref[ex.name, "low"][k * w : (k + 1) * w, :]

        @pl.when(gy < bands - 1)
        def _():
            place(pl.ds(n + 8, 8), 0, pl.ds(EDGE + rows, 8))
            for k, f in enumerate(ex.fields):
                store[f, 0, EDGE + rows : EDGE + rows + w, :] = ref[ex.name, "high"][k * w : (k + 1) * w, :]

        @pl.when(is_low)
        def _():
            for f in ex.fields:
                fill = jnp.full((8, LANES), 1.0 if f == ones else 0.0, jnp.float32)
                store[f, 0, EDGE - 8 : EDGE, :] = fill
                store[f, 1, EDGE - 8 : EDGE, :] = fill

    blane = lax.broadcasted_iota(jnp.int32, (blocks, LANES), 1)
    turn = 7 - lax.broadcasted_iota(jnp.int32, (8, LANES), 0)

    def strip_load(ex, strip):
        w, n = ex.width, ex.strip_rows
        got = ref[ex.name, "strips"]
        for k, f in enumerate(ex.fields):
            for d in range(w):
                strip[f, 2 + d] = got[pl.ds(k * w + w - 1 - d, blocks, stride=n), :]
        if ex.extra:
            perm[...] = got[pl.ds(len(ex.fields) * w, blocks, stride=n), :].astype(jnp.int32)

    def fold_rows(x):
        parts = [jnp.take_along_axis(x[b : b + 8], turn, axis=0) for b in range(blocks - 8, -1, -8)]
        index = perm[...]
        parts = [jnp.take_along_axis(p, index[8 * i : 8 * i + 8], axis=1) for i, p in enumerate(parts)]
        return jnp.concatenate(parts, axis=0)

    def fold(strip, store, fields, signs):
        for f in fields:
            for k in (0, 1):
                x = fold_rows(strip[f, 2 + k])
                strip[f, 1 - k] = -x if f in signs else x
        lane1 = lax.broadcasted_iota(jnp.int32, (1, LANES), 1)
        for f in fields:
            for k in (0, 1):
                row = slice(EDGE + rows + k, EDGE + rows + k + 1)
                store[f, 0, row, :] = strip[f, 1 - k, pl.ds(gx, 1), :]
                store[f, 1, row, :] = jnp.where(
                    lane1 < LANES // 2, strip[f, 1 - k, pl.ds(east_x, 1), :], strip[f, 1 - k, pl.ds(west_x, 1), :]
                )

    def dx_strip(x):
        a = jnp.where(blane == 0, pltpu.roll(x, blocks - 1, 0), x)
        b = jnp.where(blane == LANES - 1, pltpu.roll(x, 1, 0), x)
        return pltpu.roll(a, LANES - 1, 1) - pltpu.roll(b, 1, 1)

    def row_coriolis(i):
        row = total_rows + 1 - i
        return 0.5 * math.sin(math.pi * ((row + 0.5) / total_rows - 0.5))

    def ice_coefficients(strength, massx, cover, u, v, wx, wy):
        relax = 2.0 + jnp.sqrt(16.0 * strength / massx)
        share = cover / (1.0 + relax)
        inv = 1.0 / massx
        return share * relax, share * strength, relax, inv, u + wx * inv, v + wy * inv

    def stresses(exx, eyy, shear, c1, c2, s1, s2, s12):
        div, ten = exx + eyy, exx - eyy
        r = lax.rsqrt(div * div + (ten * ten + shear * shear) * 0.25 + 0.01)
        g = c2 * r
        return c1 * s1 + (g * div - c2), c1 * s2 + (0.25 * g) * ten, c1 * s12 + (0.125 * g) * shear

    def velocities(fx, fy, u, v, relax, inv, cover, ku, kv, ou, ov, f):
        rx, ry = ou - u, ov - v
        drag = 0.5 * jnp.sqrt(rx * rx + ry * ry)
        part = cover / (1.0 + relax + drag * inv)
        new_u = part * (relax * u + ku + inv * (fx + drag * ou) + f * v)
        new_v = part * (relax * v + kv + inv * (fy + drag * ov) - f * u)
        return new_u, new_v

    def dx_pair(m, h, first, last):
        am, ah = jnp.where(first, h, m), jnp.where(first, m, h)
        bm, bh = jnp.where(last, h, m), jnp.where(last, m, h)
        return (
            pltpu.roll(am, LANES - 1, 1) - pltpu.roll(bm, 1, 1),
            pltpu.roll(ah, LANES - 1, 1) - pltpu.roll(bh, 1, 1),
        )

    def ends(chunk):
        lane = lax.broadcasted_iota(jnp.int32, (chunk, LANES), 1)
        return lane == 0, lane == LANES - 1

    def ice_static(i):
        here = pl.ds(EDGE - 8 + i * 8, 8)
        for p in (0, 1):
            got = ice_coefficients(*(ice[f, p, here, :] for f in (STRENGTH, MASSX, COVER, U, V, WX, WY)))
            for f, x in enumerate(got):
                der[f, p, here, :] = x

    def dx_own(m, h, first, last):
        am, bm = jnp.where(first, h, m), jnp.where(last, h, m)
        return (pltpu.roll(am, LANES - 1, 1) - pltpu.roll(bm, 1, 1),)

    def ice_step(final):
        n = ICE_CHUNK
        planes, dx = ((0,), dx_own) if final else ((0, 1), dx_pair)
        first, last = ends(n)

        def stress(i):
            at = EDGE - 8 + i * n
            here, north, south = pl.ds(at, n), pl.ds(at + 1, n), pl.ds(at - 1, n)
            exx = dx_pair(ice[U, 0, here, :], ice[U, 1, here, :], first, last)
            exv = dx_pair(ice[V, 0, here, :], ice[V, 1, here, :], first, last)
            for p in (0, 1):
                eyy = ice[V, p, north, :] - ice[V, p, south, :]
                shear = ice[U, p, north, :] - ice[U, p, south, :] + exv[p]
                got = stresses(
                    exx[p], eyy, shear, der[C1, p, here, :], der[C2, p, here, :], *(ice[f, p, here, :] for f in (S1, S2, S12))
                )
                for f, x in zip((S1, S2, S12), got):
                    ice[f, p, here, :] = x

        loop(full // n, stress)

        def velocity(i):
            at = EDGE - 8 + i * n
            here, north, south = pl.ds(at, n), pl.ds(at + 1, n), pl.ds(at - 1, n)
            sums = [ice[S1, p, here, :] + ice[S2, p, here, :] for p in (0, 1)]
            dsum = dx(sums[0], sums[1], first, last)
            dxy = dx(ice[S12, 0, here, :], ice[S12, 1, here, :], first, last)
            f = cor[here, :]
            for p in planes:
                fx = 0.25 * dsum[p] + 0.5 * (ice[S12, p, north, :] - ice[S12, p, south, :])
                dyy = (ice[S1, p, north, :] - ice[S2, p, north, :]) - (ice[S1, p, south, :] - ice[S2, p, south, :])
                fy = 0.5 * dxy[p] + 0.25 * dyy
                u, v = ice[U, p, here, :], ice[V, p, here, :]
                new_u, new_v = velocities(
                    fx,
                    fy,
                    u,
                    v,
                    der[RELAX, p, here, :],
                    der[INVM, p, here, :],
                    ice[COVER, p, here, :],
                    der[KU, p, here, :],
                    der[KV, p, here, :],
                    ice[OU, p, here, :],
                    ice[OV, p, here, :],
                    f,
                )
                ice[U, p, here, :] = new_u
                ice[V, p, here, :] = new_v

        loop(full // n, velocity)

    def ice_strip_static(w):
        for i in range(1, w + 2):
            fields = (STRENGTH, MASSX, COVER, U, V, WX, WY)
            got = ice_coefficients(*(ist[f, i] for f in fields))
            for f, x in enumerate(got):
                ider[f, i] = x

    def ice_strip_step(n):
        for i in range(1, n + 1):
            exx, exv = dx_strip(ist[U, i]), dx_strip(ist[V, i])
            eyy = ist[V, i - 1] - ist[V, i + 1]
            shear = ist[U, i - 1] - ist[U, i + 1] + exv
            got = stresses(exx, eyy, shear, ider[C1, i], ider[C2, i], *(ist[f, i] for f in (S1, S2, S12)))
            for f, x in zip((S1, S2, S12), got):
                ist[f, i] = x
        for i in range(2, n):
            fx = 0.25 * dx_strip(ist[S1, i] + ist[S2, i]) + 0.5 * (ist[S12, i - 1] - ist[S12, i + 1])
            dyy = (ist[S1, i - 1] - ist[S2, i - 1]) - (ist[S1, i + 1] - ist[S2, i + 1])
            fy = 0.5 * dx_strip(ist[S12, i]) + 0.25 * dyy
            new_u, new_v = velocities(
                fx,
                fy,
                ist[U, i],
                ist[V, i],
                ider[RELAX, i],
                ider[INVM, i],
                ist[COVER, i],
                ider[KU, i],
                ider[KV, i],
                ist[OU, i],
                ist[OV, i],
                row_coriolis(i),
            )
            ist[U, i] = new_u
            ist[V, i] = new_v

    def sea_coefficients(depth, land):
        return land / (1.0 + 0.1 / depth), 0.25 * depth

    def sea_static(i):
        here = pl.ds(EDGE - 8 + i * 8, 8)
        for p in (0, 1):
            a, b = sea_coefficients(sea[DEPTH, p, here, :], sea[LAND, p, here, :])
            der[0, p, here, :] = a
            der[1, p, here, :] = b

    def flows(tu, tv, part, slope, dlx, dly, f, sx, sy):
        east = part * (tu - slope * dlx + (0.5 * f) * tv + 0.5 * sx)
        north = part * (tv - slope * dly - (0.5 * f) * tu + 0.5 * sy)
        return east, north

    def sea_step(final):
        n = SEA_CHUNK
        planes, dx = ((0,), dx_own) if final else ((0, 1), dx_pair)
        first, last = ends(n)

        def level(i):
            at = EDGE - 8 + i * n
            here, north, south = pl.ds(at, n), pl.ds(at + 1, n), pl.ds(at - 1, n)
            du = dx_pair(sea[TU, 0, here, :], sea[TU, 1, here, :], first, last)
            for p in (0, 1):
                dv = sea[TV, p, north, :] - sea[TV, p, south, :]
                sea[LEVEL, p, here, :] = sea[LAND, p, here, :] * (sea[LEVEL, p, here, :] - 0.25 * (du[p] + dv))

        loop(full // n, level)

        def flow(i):
            at = EDGE - 8 + i * n
            here, north, south = pl.ds(at, n), pl.ds(at + 1, n), pl.ds(at - 1, n)
            dlx = dx(sea[LEVEL, 0, here, :], sea[LEVEL, 1, here, :], first, last)
            f = cor[here, :]
            for p in planes:
                dly = sea[LEVEL, p, north, :] - sea[LEVEL, p, south, :]
                east, nrth = flows(
                    sea[TU, p, here, :],
                    sea[TV, p, here, :],
                    der[0, p, here, :],
                    der[1, p, here, :],
                    dlx[p],
                    dly,
                    f,
                    sea[SX, p, here, :],
                    sea[SY, p, here, :],
                )
                sea[TU, p, here, :] = east
                sea[TV, p, here, :] = nrth

        loop(full // n, flow)

    def sea_strip_static(w):
        for i in range(2, w + 2):
            a, b = sea_coefficients(sst[DEPTH, i], sst[LAND, i])
            sder[0, i] = a
            sder[1, i] = b

    def sea_strip_step(n):
        for i in range(1, n + 1):
            dv = sst[TV, i - 1] - sst[TV, i + 1]
            sst[LEVEL, i] = sst[LAND, i] * (sst[LEVEL, i] - 0.25 * (dx_strip(sst[TU, i]) + dv))
        for i in range(2, n):
            dly = sst[LEVEL, i - 1] - sst[LEVEL, i + 1]
            east, nrth = flows(
                sst[TU, i],
                sst[TV, i],
                sder[0, i],
                sder[1, i],
                dx_strip(sst[LEVEL, i]),
                dly,
                row_coriolis(i),
                sst[SX, i],
                sst[SY, i],
            )
            sst[TU, i] = east
            sst[TV, i] = nrth

    stage(ice_ex[0], ice)
    greeted = 2 + 3 * (gy < bands - 1).astype(jnp.int32) + 3 * (gy > 0).astype(jnp.int32)
    pl.semaphore_wait(barrier, greeted + (blocks - 1) * is_top.astype(jnp.int32))
    start(ice_ex[0])
    stage(sea_ex, sea)

    state = (U, V, S1, S2, S12)
    for number, ex in enumerate(ice_ex):
        if number:
            stage(ex, ice)
            start(ex)
        wait_recv(ex)
        unpack(ex, ice, MASSX)
        wait_strips(ex)
        if number == 0:
            start(sea_ex)

        @pl.when(is_top)
        def _(ex=ex, number=number):
            strip_load(ex, ist)
            fold(ist, ice, state + ((STRENGTH, MASSX, COVER, WX, WY) if number == 0 else ()), ICE_SIGNS)
            if number == 0:
                ice_strip_static(ex.width)

        if number == 0:
            loop(full // 8, ice_static)
        for step in range(ex.steps):
            if step:

                @pl.when(is_top)
                def _(n=ex.width - 2 * (step - 1)):
                    ice_strip_step(n)
                    fold(ist, ice, state, ICE_SIGNS)

            ice_step(step == ex.steps - 1)

    def surface(i):
        here = pl.ds(EDGE + i * 8, 8)
        cover = ice[COVER, 0, here, :]
        rx, ry = ice[U, 0, here, :] - ice[OU, 0, here, :], ice[V, 0, here, :] - ice[OV, 0, here, :]
        drag = cover * (0.5 * jnp.sqrt(rx * rx + ry * ry))
        sea[SX, 0, here, :] = drag * rx + (1.0 - cover) * ice[WX, 0, here, :]
        sea[SY, 0, here, :] = drag * ry + (1.0 - cover) * ice[WY, 0, here, :]

    loop(rows // 8, surface)
    stage(surf_ex, sea)
    start(surf_ex)
    outs = [
        pltpu.make_async_copy(ice.at[U : V + 1, 0, own], vel_out, out_sem.at[0]),
        pltpu.make_async_copy(ice.at[S1 : S12 + 1, 0, own], str_out, out_sem.at[1]),
        pltpu.make_async_copy(sea.at[LEVEL, 0, own], level_out, out_sem.at[2]),
        pltpu.make_async_copy(sea.at[TU : TV + 1, 0, own], trans_out, out_sem.at[3]),
    ]
    for copy in outs[:2]:
        copy.start()
    flow_state = (LEVEL, TU, TV)
    unsent = ice_ex + [sea_ex, surf_ex]
    for number, ex in enumerate([sea_ex] + later_ex):
        if number:
            stage(ex, sea)
            start(ex)
            while unsent:
                wait_send(unsent.pop())
            unsent.append(ex)
        wait_recv(ex)
        unpack(ex, sea, DEPTH)
        wait_strips(ex)

        @pl.when(is_top)
        def _(ex=ex, number=number):
            strip_load(ex, sst)
            fold(sst, sea, flow_state + ((DEPTH, LAND) if number == 0 else ()), SEA_SIGNS)
            if number == 0:
                sea_strip_static(ex.width)

        if number == 0:
            loop(full // 8, sea_static)
            wait_recv(surf_ex)
            unpack(surf_ex, sea, DEPTH)
            wait_strips(surf_ex)

            @pl.when(is_top)
            def _():
                strip_load(surf_ex, sst)

        for step in range(ex.steps):
            if step:

                @pl.when(is_top)
                def _(n=ex.width - 2 * (step - 1)):
                    sea_strip_step(n)
                    fold(sst, sea, flow_state, SEA_SIGNS)

            sea_step(step == ex.steps - 1)

    for copy in outs[2:]:
        copy.start()
    for ex in unsent:
        wait_send(ex)
    for copy in outs:
        copy.wait()


def write_out(*refs):
    sources, targets, held, sems = refs[:4], refs[4:8], refs[8:12], refs[12]
    pairs = list(zip(sources, held, targets))
    reads = [pltpu.make_async_copy(a, b, sems.at[0, i]) for i, (a, b, _) in enumerate(pairs)]
    writes = [pltpu.make_async_copy(b, c, sems.at[1, i]) for i, (_, b, c) in enumerate(pairs)]
    for copy in reads:
        copy.start()
    for read, write in zip(reads, writes):
        read.wait()
        write.start()
    for copy in writes:
        copy.wait()


def per_device(blocks, bands, *args):
    f32 = jnp.float32
    rows = args[2].shape[0]
    tall = rows + 2 * EDGE
    ice_ex, sea_ex, surf_ex, later_ex = plan(rows)
    depth = 2 + 2 * max(ICE_GROUPS + SEA_GROUPS)
    scratch = dict(
        ice=pltpu.VMEM((12, 2, tall, LANES), f32),
        der=pltpu.VMEM((6, 2, tall, LANES), f32),
        sea=pltpu.VMEM((7, 2, tall, LANES), f32),
        cor=pltpu.VMEM((tall, LANES), f32),
        ist=pltpu.VMEM((12, depth, blocks, LANES), f32),
        ider=pltpu.VMEM((6, depth, blocks, LANES), f32),
        sst=pltpu.VMEM((7, depth, blocks, LANES), f32),
        sder=pltpu.VMEM((2, depth, blocks, LANES), f32),
        masks=pltpu.VMEM((2, rows, LANES), jnp.int32),
        partner=pltpu.VMEM((1, LANES), jnp.int32),
        perm=pltpu.VMEM((blocks, LANES), jnp.int32),
        in_sem=pltpu.SemaphoreType.DMA((11,)),
        out_sem=pltpu.SemaphoreType.DMA((4,)),
    )
    for ex in ice_ex + [sea_ex, surf_ex] + later_ex:
        for part, space in ex.scratch(blocks).items():
            scratch[ex.name, part] = space

    def body(*refs):
        kernel_body(blocks, bands, list(scratch), *refs)

    sds = jax.ShapeDtypeStruct
    args = args[:-1] + (args[-1].reshape(1, LANES),)
    shapes = (
        sds((2, rows, LANES), f32),
        sds((3, rows, LANES), f32),
        sds((rows, LANES), f32),
        sds((2, rows, LANES), f32),
    )
    far = pl.BlockSpec(memory_space=pltpu.HBM)
    results = pl.pallas_call(
        body,
        out_shape=shapes,
        in_specs=[far] * 11,
        out_specs=(far,) * 4,
        scratch_shapes=list(scratch.values()),
        compiler_params=pltpu.CompilerParams(
            collective_id=0, has_side_effects=True, vmem_limit_bytes=67043328
        ),
        name="coupled_step",
    )(*args)
    return pl.pallas_call(
        write_out,
        out_shape=shapes,
        in_specs=[far] * 4,
        out_specs=(far,) * 4,
        scratch_shapes=[pltpu.VMEM(x.shape, f32) for x in shapes] + [pltpu.SemaphoreType.DMA((2, 4))],
        compiler_params=pltpu.CompilerParams(vmem_limit_bytes=67043328),
        name="write_out",
    )(*results)


def solution(mesh):
    blocks, bands = mesh.shape["gx"], mesh.shape["gy"]
    flat, stacked = P("gy", "gx"), P(None, "gy", "gx")
    in_specs = (stacked, stacked, flat, flat, stacked, flat, stacked, flat, flat, flat, P("gx"))

    def step(*args):
        return per_device(blocks, bands, *args)

    return jax.shard_map(
        step, mesh=mesh, in_specs=in_specs, out_specs=(stacked, stacked, flat, stacked), check_vma=False
    )
```

```python
import math

import jax
import jax.numpy as jnp
from jax import lax
from jax.experimental import pallas as pl
from jax.experimental.pallas import tpu as pltpu
from jax.sharding import PartitionSpec as P

ICE_GROUPS = (4,)
SEA_GROUPS = (3, 3)
EDGE = 16
ICE_CHUNK = 24
SEA_CHUNK = 24
LANES = 128
MESH_ID = pl.DeviceIdType.MESH

U, V, S1, S2, S12, STRENGTH, MASSX, COVER, WX, WY, OU, OV = range(12)
C1, C2, RELAX, INVM, KU, KV = range(6)
LEVEL, TU, TV, DEPTH, LAND, SX, SY = range(7)
ICE_SIGNS = {U: -1.0, V: -1.0}
SEA_SIGNS = {TU: -1.0, TV: -1.0}


class Exchange:
    def __init__(self, name, fields, steps, rows):
        self.name, self.fields, self.steps = name, fields, steps
        self.width = 2 * steps
        lanes = len(fields) * self.width
        self.groups = 4 if lanes <= 32 else 2 if lanes <= 64 else 1
        self.group_lanes = LANES // self.groups
        assert len(fields) * self.width <= self.group_lanes
        self.group_rows = rows // self.groups
        self.extra = name == "ice0"
        count = len(fields) * self.width + (1 if self.extra else 0)
        self.strip_rows = -(-count // 8) * 8

    def scratch(self, blocks):
        f32 = jnp.float32
        packed, got = (self.group_rows, LANES), (self.group_rows + 16, LANES)
        strip = (self.strip_rows, LANES)
        return dict(
            top=pltpu.VMEM(strip, f32),
            bot=pltpu.VMEM(strip, f32),
            low=pltpu.VMEM(strip, f32),
            high=pltpu.VMEM(strip, f32),
            west=pltpu.VMEM(packed, f32),
            east=pltpu.VMEM(packed, f32),
            right=pltpu.VMEM(got, f32),
            left=pltpu.VMEM(got, f32),
            strips=pltpu.VMEM((blocks * self.strip_rows, LANES), f32),
            send=pltpu.SemaphoreType.DMA((8,)),
            recv=pltpu.SemaphoreType.DMA((8,)),
            strip_send=pltpu.SemaphoreType.DMA((blocks,)),
            strip_recv=pltpu.SemaphoreType.DMA((blocks,)),
        )


def plan(rows):
    ice = [Exchange(f"ice{i}", list(range(12 if i == 0 else 5)), s, rows) for i, s in enumerate(ICE_GROUPS)]
    first = Exchange("sea0", [LEVEL, TU, TV, DEPTH, LAND], SEA_GROUPS[0], rows)
    surf = Exchange("surf", [SX, SY], SEA_GROUPS[0], rows)
    later = [Exchange(f"sea{i}", [LEVEL, TU, TV], s, rows) for i, s in enumerate(SEA_GROUPS) if i]
    return ice, first, surf, later


def kernel_body(
    blocks,
    bands,
    names,
    vel_in,
    str_in,
    mass_in,
    strength_in,
    wind_in,
    level_in,
    trans_in,
    depth_in,
    land_in,
    icemask_in,
    partner_in,
    vel_out,
    str_out,
    level_out,
    trans_out,
    *scratch,
):
    ref = dict(zip(names, scratch))
    ice, der, sea, cor = ref["ice"], ref["der"], ref["sea"], ref["cor"]
    ist, ider, sst, sder = ref["ist"], ref["ider"], ref["sst"], ref["sder"]
    masks, partner, perm = ref["masks"], ref["partner"], ref["perm"]
    in_sem, out_sem = ref["in_sem"], ref["out_sem"]
    rows = mass_in.shape[0]
    total_rows = rows * bands
    own = slice(EDGE, EDGE + rows)
    full = rows + 16
    gy, gx = lax.axis_index("gy"), lax.axis_index("gx")
    west_x, east_x = lax.rem(gx + blocks - 1, blocks), lax.rem(gx + 1, blocks)
    is_top, is_low = gy == bands - 1, gy == 0
    ice_ex, sea_ex, surf_ex, later_ex = plan(rows)

    barrier = pltpu.get_barrier_semaphore()

    def greet(y, x):
        pl.semaphore_signal(barrier, inc=1, device_id=(y, x), device_id_type=MESH_ID)

    greet(gy, west_x)
    greet(gy, east_x)

    @pl.when(gy < bands - 1)
    def _():
        for x in (gx, west_x, east_x):
            greet(gy + 1, x)

    @pl.when(gy > 0)
    def _():
        for x in (gx, west_x, east_x):
            greet(gy - 1, x)

    @pl.when(is_top)
    def _():
        def one(j, carry):
            greet(gy, lax.rem(gx + j, blocks))
            return carry

        lax.fori_loop(1, blocks, one, 0)

    loads = [
        (vel_in, ice.at[U : V + 1, 0, own]),
        (str_in, ice.at[S1 : S12 + 1, 0, own]),
        (mass_in, ice.at[MASSX, 0, own]),
        (strength_in, ice.at[STRENGTH, 0, own]),
        (wind_in, ice.at[WX : WY + 1, 0, own]),
        (level_in, sea.at[LEVEL, 0, own]),
        (trans_in, sea.at[TU : TV + 1, 0, own]),
        (depth_in, sea.at[DEPTH, 0, own]),
        (land_in, masks.at[0]),
        (icemask_in, masks.at[1]),
        (partner_in, partner),
    ]
    loads = [pltpu.make_async_copy(a, b, in_sem.at[i]) for i, (a, b) in enumerate(loads)]
    for copy in loads:
        copy.start()

    def loop(count, body):
        for i in range(count):
            body(i)

    def coriolis(i):
        at = i * 8
        r = lax.broadcasted_iota(jnp.int32, (8, LANES), 0) + (gy * rows + at - EDGE)
        angle = jnp.pi * ((r.astype(jnp.float32) + 0.5) / total_rows - 0.5)
        cor[pl.ds(at, 8), :] = 0.5 * jnp.sin(angle)

    loop((rows + 2 * EDGE) // 8, coriolis)
    for copy in loads:
        copy.wait()

    def prepare(i):
        at = i * 8
        here, m = pl.ds(at + EDGE, 8), pl.ds(at, 8)
        land = masks[0, m, :].astype(jnp.float32)
        cover = land * masks[1, m, :].astype(jnp.float32)
        depth = sea[DEPTH, 0, here, :]
        sea[LAND, 0, here, :] = land
        ice[COVER, 0, here, :] = cover
        ice[MASSX, 0, here, :] = ice[MASSX, 0, here, :] + 1.0 - cover
        ice[OU, 0, here, :] = sea[TU, 0, here, :] / depth
        ice[OV, 0, here, :] = sea[TV, 0, here, :] / depth

    loop(rows // 8, prepare)

    lane8 = lax.broadcasted_iota(jnp.int32, (8, LANES), 1)

    def stage(ex, store):
        w = ex.width
        top, bot = ref[ex.name, "top"], ref[ex.name, "bot"]
        for k, f in enumerate(ex.fields):
            top[k * w : (k + 1) * w, :] = store[f, 0, EDGE + rows - w : EDGE + rows, :]
            bot[k * w : (k + 1) * w, :] = store[f, 0, EDGE : EDGE + w, :]
        if ex.extra:
            at = len(ex.fields) * w
            local = partner[...] - (blocks - 1 - gx) * LANES
            top[at : at + 1, :] = local.astype(jnp.float32)

        def pack(i):
            to_west = to_east = None
            for g in range(ex.groups):
                for k, f in enumerate(ex.fields):
                    at = g * ex.group_lanes + k * w
                    here = pl.ds(EDGE + g * ex.group_rows + i * 8, 8)
                    x = store[f, 0, here, :]
                    a = pltpu.roll(x, at, 1) if at else x
                    b = pltpu.roll(x, (at + w) % LANES, 1) if (at + w) % LANES else x
                    if to_west is None:
                        to_west, to_east = a, b
                    else:
                        keep = lane8 < at
                        to_west = jnp.where(keep, to_west, a)
                        to_east = jnp.where(keep, to_east, b)
            m = pl.ds(i * 8, 8)
            ref[ex.name, "west"][m, :] = to_west
            ref[ex.name, "east"][m, :] = to_east

        loop(ex.group_rows // 8, pack)

    def sends(ex):
        r = lambda part: ref[ex.name, part]
        n = ex.group_rows
        last, first = pl.ds(n - 8, 8), pl.ds(0, 8)
        mid, low, high = pl.ds(0, n), pl.ds(n, 8), pl.ds(n + 8, 8)
        up, down, flat = 1, -1, 0
        table = [
            (r("top"), r("low"), up, gx),
            (r("bot"), r("high"), down, gx),
            (r("west"), r("right").at[mid], flat, west_x),
            (r("east"), r("left").at[mid], flat, east_x),
            (r("west").at[last], r("right").at[low], up, west_x),
            (r("east").at[last], r("left").at[low], up, east_x),
            (r("west").at[first], r("right").at[high], down, west_x),
            (r("east").at[first], r("left").at[high], down, east_x),
        ]
        out = []
        for i, (src, dst, dy, x) in enumerate(table):
            copy = pltpu.make_async_remote_copy(
                src_ref=src,
                dst_ref=dst,
                send_sem=r("send").at[i],
                recv_sem=r("recv").at[i],
                device_id=(gy + dy, x),
                device_id_type=MESH_ID,
            )
            out.append((dy, copy))
        return out

    def strip_copy(ex, target, source):
        n = ex.strip_rows
        return pltpu.make_async_remote_copy(
            src_ref=ref[ex.name, "top"],
            dst_ref=ref[ex.name, "strips"].at[pl.ds(pl.multiple_of(source * n, 8), n)],
            send_sem=ref[ex.name, "strip_send"].at[target],
            recv_sem=ref[ex.name, "strip_recv"].at[source],
            device_id=(gy, target),
            device_id_type=MESH_ID,
        )

    def each_strip(ex, action):
        reach = ex.steps

        @pl.when(is_top)
        def _():
            for j in range(1, blocks):
                x = lax.rem(gx + j, blocks)
                if j <= reach or j >= blocks - reach:
                    action(x)
                else:
                    gap = lax.rem(x + gx + 1, blocks)
                    pl.when((gap <= reach) | (gap >= blocks - reach))(lambda x=x: action(x))

    def start(ex):
        each_strip(ex, lambda x: strip_copy(ex, x, gx).start())
        copies = sends(ex)
        for dy in (0, 1, -1):
            chosen = [c for d, c in copies if d == dy]

            def go(chosen=chosen):
                for c in chosen:
                    c.start()

            if dy == 0:
                go()
            else:
                pl.when((gy < bands - 1) if dy > 0 else (gy > 0))(go)
        n = ex.strip_rows

        @pl.when(is_top)
        def _():
            ref[ex.name, "strips"][pl.ds(pl.multiple_of(gx * n, 8), n), :] = ref[ex.name, "top"][...]

    def wait_recv(ex):
        copies = sends(ex)
        for dy in (0, 1, -1):
            chosen = [c for d, c in copies if d == dy]

            def go(chosen=chosen):
                for c in chosen:
                    c.wait_recv()

            if dy == 0:
                go()
            else:
                pl.when((gy > 0) if dy > 0 else (gy < bands - 1))(go)

    def wait_strips(ex):
        each_strip(ex, lambda x: strip_copy(ex, gx, x).wait_recv())

    def wait_send(ex):
        copies = sends(ex)
        for dy in (0, 1, -1):
            chosen = [c for d, c in copies if d == dy]

            def go(chosen=chosen):
                for c in chosen:
                    c.wait_send()

            if dy == 0:
                go()
            else:
                pl.when((gy < bands - 1) if dy > 0 else (gy > 0))(go)
        each_strip(ex, lambda x: strip_copy(ex, x, gx).wait_send())

    def unpack(ex, store, ones):
        w, n = ex.width, ex.group_rows
        right, left = ref[ex.name, "right"], ref[ex.name, "left"]

        def place(source, g, target):
            x, y = right[source, :], left[source, :]
            for k, f in enumerate(ex.fields):
                at = g * ex.group_lanes + k * w
                a = pltpu.roll(x, (LANES - at) % LANES, 1) if at else x
                shift = (2 * LANES - w - at) % LANES
                b = pltpu.roll(y, shift, 1) if shift else y
                store[f, 1, target, :] = jnp.where(lane8 < LANES // 2, a, b)

        def main(i):
            source = pl.ds(i * 8, 8)
            for g in range(ex.groups):
                place(source, g, pl.ds(EDGE + g * n + i * 8, 8))

        loop(n // 8, main)

        @pl.when(gy > 0)
        def _():
            place(pl.ds(n, 8), ex.groups - 1, pl.ds(EDGE - 8, 8))
            for k, f in enumerate(ex.fields):
                store[f, 0, EDGE - w : EDGE, :] = ref[ex.name, "low"][k * w : (k + 1) * w, :]

        @pl.when(gy < bands - 1)
        def _():
            place(pl.ds(n + 8, 8), 0, pl.ds(EDGE + rows, 8))
            for k, f in enumerate(ex.fields):
                store[f, 0, EDGE + rows : EDGE + rows + w, :] = ref[ex.name, "high"][k * w : (k + 1) * w, :]

        @pl.when(is_low)
        def _():
            for f in ex.fields:
                fill = jnp.full((8, LANES), 1.0 if f == ones else 0.0, jnp.float32)
                store[f, 0, EDGE - 8 : EDGE, :] = fill
                store[f, 1, EDGE - 8 : EDGE, :] = fill

    blane = lax.broadcasted_iota(jnp.int32, (blocks, LANES), 1)
    turn = 7 - lax.broadcasted_iota(jnp.int32, (8, LANES), 0)

    def strip_load(ex, strip):
        w, n = ex.width, ex.strip_rows
        got = ref[ex.name, "strips"]
        for k, f in enumerate(ex.fields):
            for d in range(w):
                strip[f, 2 + d] = got[pl.ds(k * w + w - 1 - d, blocks, stride=n), :]
        if ex.extra:
            perm[...] = got[pl.ds(len(ex.fields) * w, blocks, stride=n), :].astype(jnp.int32)

    def fold_rows(x):
        parts = [jnp.take_along_axis(x[b : b + 8], turn, axis=0) for b in range(blocks - 8, -1, -8)]
        index = perm[...]
        parts = [jnp.take_along_axis(p, index[8 * i : 8 * i + 8], axis=1) for i, p in enumerate(parts)]
        return jnp.concatenate(parts, axis=0)

    def fold(strip, store, fields, signs):
        for f in fields:
            for k in (0, 1):
                x = fold_rows(strip[f, 2 + k])
                strip[f, 1 - k] = -x if f in signs else x
        lane1 = lax.broadcasted_iota(jnp.int32, (1, LANES), 1)
        for f in fields:
            for k in (0, 1):
                row = slice(EDGE + rows + k, EDGE + rows + k + 1)
                store[f, 0, row, :] = strip[f, 1 - k, pl.ds(gx, 1), :]
                store[f, 1, row, :] = jnp.where(
                    lane1 < LANES // 2, strip[f, 1 - k, pl.ds(east_x, 1), :], strip[f, 1 - k, pl.ds(west_x, 1), :]
                )

    def dx_strip(x):
        a = jnp.where(blane == 0, pltpu.roll(x, blocks - 1, 0), x)
        b = jnp.where(blane == LANES - 1, pltpu.roll(x, 1, 0), x)
        return pltpu.roll(a, LANES - 1, 1) - pltpu.roll(b, 1, 1)

    def row_coriolis(i):
        row = total_rows + 1 - i
        return 0.5 * math.sin(math.pi * ((row + 0.5) / total_rows - 0.5))

    def ice_coefficients(strength, massx, cover, u, v, wx, wy):
        relax = 2.0 + jnp.sqrt(16.0 * strength / massx)
        share = cover / (1.0 + relax)
        inv = 1.0 / massx
        return share * relax, share * strength, relax, inv, u + wx * inv, v + wy * inv

    def stresses(exx, eyy, shear, c1, c2, s1, s2, s12):
        div, ten = exx + eyy, exx - eyy
        r = lax.rsqrt(div * div + (ten * ten + shear * shear) * 0.25 + 0.01)
        g = c2 * r
        return c1 * s1 + (g * div - c2), c1 * s2 + (0.25 * g) * ten, c1 * s12 + (0.125 * g) * shear

    def velocities(fx, fy, u, v, relax, inv, cover, ku, kv, ou, ov, f):
        rx, ry = ou - u, ov - v
        drag = 0.5 * jnp.sqrt(rx * rx + ry * ry)
        part = cover / (1.0 + relax + drag * inv)
        new_u = part * (relax * u + ku + inv * (fx + drag * ou) + f * v)
        new_v = part * (relax * v + kv + inv * (fy + drag * ov) - f * u)
        return new_u, new_v

    def dx_pair(m, h, first, last):
        am, ah = jnp.where(first, h, m), jnp.where(first, m, h)
        bm, bh = jnp.where(last, h, m), jnp.where(last, m, h)
        return (
            pltpu.roll(am, LANES - 1, 1) - pltpu.roll(bm, 1, 1),
            pltpu.roll(ah, LANES - 1, 1) - pltpu.roll(bh, 1, 1),
        )

    def ends(chunk):
        lane = lax.broadcasted_iota(jnp.int32, (chunk, LANES), 1)
        return lane == 0, lane == LANES - 1

    def ice_static(i):
        here = pl.ds(EDGE - 8 + i * 8, 8)
        for p in (0, 1):
            got = ice_coefficients(*(ice[f, p, here, :] for f in (STRENGTH, MASSX, COVER, U, V, WX, WY)))
            for f, x in enumerate(got):
                der[f, p, here, :] = x

    def dx_own(m, h, first, last):
        am, bm = jnp.where(first, h, m), jnp.where(last, h, m)
        return (pltpu.roll(am, LANES - 1, 1) - pltpu.roll(bm, 1, 1),)

    def ice_step(final):
        n = ICE_CHUNK
        planes, dx = ((0,), dx_own) if final else ((0, 1), dx_pair)
        first, last = ends(n)

        def stress(i):
            at = EDGE - 8 + i * n
            here, north, south = pl.ds(at, n), pl.ds(at + 1, n), pl.ds(at - 1, n)
            exx = dx_pair(ice[U, 0, here, :], ice[U, 1, here, :], first, last)
            exv = dx_pair(ice[V, 0, here, :], ice[V, 1, here, :], first, last)
            for p in (0, 1):
                eyy = ice[V, p, north, :] - ice[V, p, south, :]
                shear = ice[U, p, north, :] - ice[U, p, south, :] + exv[p]
                got = stresses(
                    exx[p], eyy, shear, der[C1, p, here, :], der[C2, p, here, :], *(ice[f, p, here, :] for f in (S1, S2, S12))
                )
                for f, x in zip((S1, S2, S12), got):
                    ice[f, p, here, :] = x

        loop(full // n, stress)

        def velocity(i):
            at = EDGE - 8 + i * n
            here, north, south = pl.ds(at, n), pl.ds(at + 1, n), pl.ds(at - 1, n)
            sums = [ice[S1, p, here, :] + ice[S2, p, here, :] for p in (0, 1)]
            dsum = dx(sums[0], sums[1], first, last)
            dxy = dx(ice[S12, 0, here, :], ice[S12, 1, here, :], first, last)
            f = cor[here, :]
            for p in planes:
                fx = 0.25 * dsum[p] + 0.5 * (ice[S12, p, north, :] - ice[S12, p, south, :])
                dyy = (ice[S1, p, north, :] - ice[S2, p, north, :]) - (ice[S1, p, south, :] - ice[S2, p, south, :])
                fy = 0.5 * dxy[p] + 0.25 * dyy
                u, v = ice[U, p, here, :], ice[V, p, here, :]
                new_u, new_v = velocities(
                    fx,
                    fy,
                    u,
                    v,
                    der[RELAX, p, here, :],
                    der[INVM, p, here, :],
                    ice[COVER, p, here, :],
                    der[KU, p, here, :],
                    der[KV, p, here, :],
                    ice[OU, p, here, :],
                    ice[OV, p, here, :],
                    f,
                )
                ice[U, p, here, :] = new_u
                ice[V, p, here, :] = new_v

        loop(full // n, velocity)

    def ice_strip_static(w):
        for i in range(1, w + 2):
            fields = (STRENGTH, MASSX, COVER, U, V, WX, WY)
            got = ice_coefficients(*(ist[f, i] for f in fields))
            for f, x in enumerate(got):
                ider[f, i] = x

    def ice_strip_step(n):
        for i in range(1, n + 1):
            exx, exv = dx_strip(ist[U, i]), dx_strip(ist[V, i])
            eyy = ist[V, i - 1] - ist[V, i + 1]
            shear = ist[U, i - 1] - ist[U, i + 1] + exv
            got = stresses(exx, eyy, shear, ider[C1, i], ider[C2, i], *(ist[f, i] for f in (S1, S2, S12)))
            for f, x in zip((S1, S2, S12), got):
                ist[f, i] = x
        for i in range(2, n):
            fx = 0.25 * dx_strip(ist[S1, i] + ist[S2, i]) + 0.5 * (ist[S12, i - 1] - ist[S12, i + 1])
            dyy = (ist[S1, i - 1] - ist[S2, i - 1]) - (ist[S1, i + 1] - ist[S2, i + 1])
            fy = 0.5 * dx_strip(ist[S12, i]) + 0.25 * dyy
            new_u, new_v = velocities(
                fx,
                fy,
                ist[U, i],
                ist[V, i],
                ider[RELAX, i],
                ider[INVM, i],
                ist[COVER, i],
                ider[KU, i],
                ider[KV, i],
                ist[OU, i],
                ist[OV, i],
                row_coriolis(i),
            )
            ist[U, i] = new_u
            ist[V, i] = new_v

    def sea_coefficients(depth, land):
        return land / (1.0 + 0.1 / depth), 0.25 * depth

    def sea_static(i):
        here = pl.ds(EDGE - 8 + i * 8, 8)
        for p in (0, 1):
            a, b = sea_coefficients(sea[DEPTH, p, here, :], sea[LAND, p, here, :])
            der[0, p, here, :] = a
            der[1, p, here, :] = b

    def flows(tu, tv, part, slope, dlx, dly, f, sx, sy):
        east = part * (tu - slope * dlx + (0.5 * f) * tv + 0.5 * sx)
        north = part * (tv - slope * dly - (0.5 * f) * tu + 0.5 * sy)
        return east, north

    def sea_step(final):
        n = SEA_CHUNK
        planes, dx = ((0,), dx_own) if final else ((0, 1), dx_pair)
        first, last = ends(n)

        def level(i):
            at = EDGE - 8 + i * n
            here, north, south = pl.ds(at, n), pl.ds(at + 1, n), pl.ds(at - 1, n)
            du = dx_pair(sea[TU, 0, here, :], sea[TU, 1, here, :], first, last)
            for p in (0, 1):
                dv = sea[TV, p, north, :] - sea[TV, p, south, :]
                sea[LEVEL, p, here, :] = sea[LAND, p, here, :] * (sea[LEVEL, p, here, :] - 0.25 * (du[p] + dv))

        loop(full // n, level)

        def flow(i):
            at = EDGE - 8 + i * n
            here, north, south = pl.ds(at, n), pl.ds(at + 1, n), pl.ds(at - 1, n)
            dlx = dx(sea[LEVEL, 0, here, :], sea[LEVEL, 1, here, :], first, last)
            f = cor[here, :]
            for p in planes:
                dly = sea[LEVEL, p, north, :] - sea[LEVEL, p, south, :]
                east, nrth = flows(
                    sea[TU, p, here, :],
                    sea[TV, p, here, :],
                    der[0, p, here, :],
                    der[1, p, here, :],
                    dlx[p],
                    dly,
                    f,
                    sea[SX, p, here, :],
                    sea[SY, p, here, :],
                )
                sea[TU, p, here, :] = east
                sea[TV, p, here, :] = nrth

        loop(full // n, flow)

    def sea_strip_static(w):
        for i in range(2, w + 2):
            a, b = sea_coefficients(sst[DEPTH, i], sst[LAND, i])
            sder[0, i] = a
            sder[1, i] = b

    def sea_strip_step(n):
        for i in range(1, n + 1):
            dv = sst[TV, i - 1] - sst[TV, i + 1]
            sst[LEVEL, i] = sst[LAND, i] * (sst[LEVEL, i] - 0.25 * (dx_strip(sst[TU, i]) + dv))
        for i in range(2, n):
            dly = sst[LEVEL, i - 1] - sst[LEVEL, i + 1]
            east, nrth = flows(
                sst[TU, i],
                sst[TV, i],
                sder[0, i],
                sder[1, i],
                dx_strip(sst[LEVEL, i]),
                dly,
                row_coriolis(i),
                sst[SX, i],
                sst[SY, i],
            )
            sst[TU, i] = east
            sst[TV, i] = nrth

    stage(ice_ex[0], ice)
    greeted = 2 + 3 * (gy < bands - 1).astype(jnp.int32) + 3 * (gy > 0).astype(jnp.int32)
    pl.semaphore_wait(barrier, greeted + (blocks - 1) * is_top.astype(jnp.int32))
    start(ice_ex[0])
    stage(sea_ex, sea)

    state = (U, V, S1, S2, S12)
    for number, ex in enumerate(ice_ex):
        if number:
            stage(ex, ice)
            start(ex)
        wait_recv(ex)
        unpack(ex, ice, MASSX)
        wait_strips(ex)
        if number == 0:
            start(sea_ex)

        @pl.when(is_top)
        def _(ex=ex, number=number):
            strip_load(ex, ist)
            fold(ist, ice, state + ((STRENGTH, MASSX, COVER, WX, WY) if number == 0 else ()), ICE_SIGNS)
            if number == 0:
                ice_strip_static(ex.width)

        if number == 0:
            loop(full // 8, ice_static)
        for step in range(ex.steps):
            if step:

                @pl.when(is_top)
                def _(n=ex.width - 2 * (step - 1)):
                    ice_strip_step(n)
                    fold(ist, ice, state, ICE_SIGNS)

            ice_step(step == ex.steps - 1)

    def surface(i):
        here = pl.ds(EDGE + i * 8, 8)
        cover = ice[COVER, 0, here, :]
        rx, ry = ice[U, 0, here, :] - ice[OU, 0, here, :], ice[V, 0, here, :] - ice[OV, 0, here, :]
        drag = cover * (0.5 * jnp.sqrt(rx * rx + ry * ry))
        sea[SX, 0, here, :] = drag * rx + (1.0 - cover) * ice[WX, 0, here, :]
        sea[SY, 0, here, :] = drag * ry + (1.0 - cover) * ice[WY, 0, here, :]

    loop(rows // 8, surface)
    stage(surf_ex, sea)
    start(surf_ex)
    outs = [
        pltpu.make_async_copy(ice.at[U : V + 1, 0, own], vel_out, out_sem.at[0]),
        pltpu.make_async_copy(ice.at[S1 : S12 + 1, 0, own], str_out, out_sem.at[1]),
        pltpu.make_async_copy(sea.at[LEVEL, 0, own], level_out, out_sem.at[2]),
        pltpu.make_async_copy(sea.at[TU : TV + 1, 0, own], trans_out, out_sem.at[3]),
    ]
    for copy in outs[:2]:
        copy.start()
    flow_state = (LEVEL, TU, TV)
    unsent = ice_ex + [sea_ex, surf_ex]
    for number, ex in enumerate([sea_ex] + later_ex):
        if number:
            stage(ex, sea)
            start(ex)
            while unsent:
                wait_send(unsent.pop())
            unsent.append(ex)
        wait_recv(ex)
        unpack(ex, sea, DEPTH)
        wait_strips(ex)

        @pl.when(is_top)
        def _(ex=ex, number=number):
            strip_load(ex, sst)
            fold(sst, sea, flow_state + ((DEPTH, LAND) if number == 0 else ()), SEA_SIGNS)
            if number == 0:
                sea_strip_static(ex.width)

        if number == 0:
            loop(full // 8, sea_static)
            wait_recv(surf_ex)
            unpack(surf_ex, sea, DEPTH)
            wait_strips(surf_ex)

            @pl.when(is_top)
            def _():
                strip_load(surf_ex, sst)

        for step in range(ex.steps):
            if step:

                @pl.when(is_top)
                def _(n=ex.width - 2 * (step - 1)):
                    sea_strip_step(n)
                    fold(sst, sea, flow_state, SEA_SIGNS)

            sea_step(step == ex.steps - 1)

    for copy in outs[2:]:
        copy.start()
    for ex in unsent:
        wait_send(ex)
    for copy in outs:
        copy.wait()


def write_out(*refs):
    sources, targets, held, sems = refs[:4], refs[4:8], refs[8:12], refs[12]
    pairs = list(zip(sources, held, targets))
    reads = [pltpu.make_async_copy(a, b, sems.at[0, i]) for i, (a, b, _) in enumerate(pairs)]
    writes = [pltpu.make_async_copy(b, c, sems.at[1, i]) for i, (_, b, c) in enumerate(pairs)]
    for copy in reads:
        copy.start()
    for read, write in zip(reads, writes):
        read.wait()
        write.start()
    for copy in writes:
        copy.wait()


def per_device(blocks, bands, *args):
    f32 = jnp.float32
    rows = args[2].shape[0]
    tall = rows + 2 * EDGE
    ice_ex, sea_ex, surf_ex, later_ex = plan(rows)
    depth = 2 + 2 * max(ICE_GROUPS + SEA_GROUPS)
    scratch = dict(
        ice=pltpu.VMEM((12, 2, tall, LANES), f32),
        der=pltpu.VMEM((6, 2, tall, LANES), f32),
        sea=pltpu.VMEM((7, 2, tall, LANES), f32),
        cor=pltpu.VMEM((tall, LANES), f32),
        ist=pltpu.VMEM((12, depth, blocks, LANES), f32),
        ider=pltpu.VMEM((6, depth, blocks, LANES), f32),
        sst=pltpu.VMEM((7, depth, blocks, LANES), f32),
        sder=pltpu.VMEM((2, depth, blocks, LANES), f32),
        masks=pltpu.VMEM((2, rows, LANES), jnp.int32),
        partner=pltpu.VMEM((1, LANES), jnp.int32),
        perm=pltpu.VMEM((blocks, LANES), jnp.int32),
        in_sem=pltpu.SemaphoreType.DMA((11,)),
        out_sem=pltpu.SemaphoreType.DMA((4,)),
    )
    for ex in ice_ex + [sea_ex, surf_ex] + later_ex:
        for part, space in ex.scratch(blocks).items():
            scratch[ex.name, part] = space

    def body(*refs):
        kernel_body(blocks, bands, list(scratch), *refs)

    sds = jax.ShapeDtypeStruct
    args = args[:-1] + (args[-1].reshape(1, LANES),)
    shapes = (
        sds((2, rows, LANES), f32),
        sds((3, rows, LANES), f32),
        sds((rows, LANES), f32),
        sds((2, rows, LANES), f32),
    )
    far = pl.BlockSpec(memory_space=pltpu.HBM)
    results = pl.pallas_call(
        body,
        out_shape=shapes,
        in_specs=[far] * 11,
        out_specs=(far,) * 4,
        scratch_shapes=list(scratch.values()),
        compiler_params=pltpu.CompilerParams(
            collective_id=0, has_side_effects=True, vmem_limit_bytes=67043328
        ),
        name="coupled_step",
    )(*args)
    return pl.pallas_call(
        write_out,
        out_shape=shapes,
        in_specs=[far] * 4,
        out_specs=(far,) * 4,
        scratch_shapes=[pltpu.VMEM(x.shape, f32) for x in shapes] + [pltpu.SemaphoreType.DMA((2, 4))],
        compiler_params=pltpu.CompilerParams(vmem_limit_bytes=67043328),
        name="write_out",
    )(*results)


def solution(mesh):
    blocks, bands = mesh.shape["gx"], mesh.shape["gy"]
    flat, stacked = P("gy", "gx"), P(None, "gy", "gx")
    in_specs = (stacked, stacked, flat, flat, stacked, flat, stacked, flat, flat, flat, P("gx"))

    def step(*args):
        return per_device(blocks, bands, *args)

    return jax.shard_map(
        step, mesh=mesh, in_specs=in_specs, out_specs=(stacked, stacked, flat, stacked), check_vma=False
    )
```
